32 devices in a mesh: replica: 4 (over z), fsdp: 8 (over y, x, core).
Axes of the slice: x: 2, y: 2, z: 4, core: 2. Of those that a mesh axis runs over, the one named last changes fastest.
Arguments:
- states: bfloat16 [32, 256, 2048], P(('replica', 'fsdp'))
- cotangent: bfloat16 [32, 256, 512], P(('replica', 'fsdp')), may hold values from -6 to 6
- kv_weight: bfloat16 [2048, 512], P('fsdp'), may hold values from -0.125 to 0.125
- norm_gain: bfloat16 [2048], P('fsdp'), may hold values from -1.5 to 1.5
- prompt_len: int32 [32], P(('replica', 'fsdp')), may hold values from 1 to 255, as said below
- response_len: int32 [32], P(('replica', 'fsdp')), may hold values from 1 to 192
- reward_bucket: int32 [32], P(('replica', 'fsdp')), may hold values from 0 to 10, as said below
Outputs:
- key_values: bfloat16 [32, 256, 512], P(('replica', 'fsdp'))
- grad_weight: float32 [2048, 512], P('fsdp')
- grad_gain: float32 [2048], P('fsdp')
The draws below stay inside these ranges and needn't reach their ends.
Inputs may be any that keep to these rules, and one draw needn't show every extreme that they name: prompt_len + response_len <= 256 for every rollout. `reward_bucket`: some rollout has level 0 and some has level 10.
All inputs are finite; a program needn't handle non-finite values.
Results may differ from the reference program's by a relative error of at most 0.005.
Values may be sent and summed in bfloat16 or wider, within the bound.
A program may use at most 64 MiB of HBM per device.

```python
import math
import jax
import jax.numpy as jnp
from jax import lax

D = 2048
KV = 512
SEQ = 256
BUCKETS = 11
ROLLOUTS = 32


def lengths_pair(key):
    salted = jax.random.fold_in(key, 101)
    key_length, key_prompt = jax.random.split(salted)
    rollout_index = jnp.arange(ROLLOUTS, dtype=jnp.int32)
    ceiling = SEQ // 4 + SEQ // 2 * rollout_index // max(ROLLOUTS - 1, 1)
    response = 1 + jax.random.randint(key_length, (ROLLOUTS,), 0, ceiling, dtype=jnp.int32)
    response = response.at[ROLLOUTS - 1].set(SEQ // 4 + SEQ // 2).at[0].set(1)
    prompt = 1 + jax.random.randint(key_prompt, (ROLLOUTS,), 0, SEQ - response, dtype=jnp.int32)
    prompt = prompt.at[0].set(SEQ - 1)
    return (prompt, response)


def draw_prompt_len(key, part):
    return lengths_pair(key)[0]


def draw_response_len(key, part):
    return lengths_pair(key)[1]


def draw_reward_bucket(key, part):
    salted = jax.random.fold_in(key, 202)
    rollout_index = jnp.arange(ROLLOUTS, dtype=jnp.int32)
    ceiling = BUCKETS // 3 + (BUCKETS - BUCKETS // 3) * rollout_index // max(ROLLOUTS - 1, 1)
    levels = jax.random.randint(salted, (ROLLOUTS,), 0, ceiling, dtype=jnp.int32)
    return levels.at[0].set(0).at[ROLLOUTS - 1].set(BUCKETS - 1)


def draw_states(key, part):
    salted = jax.random.fold_in(key, 303)
    key_base, key_rows, key_columns = jax.random.split(salted, 3)
    base = jax.random.normal(key_base, (ROLLOUTS, SEQ, D), jnp.float32)
    row_scale = jnp.exp(jax.random.uniform(key_rows, (ROLLOUTS, SEQ, 1), jnp.float32, math.log(0.3), math.log(3.0)))
    column_scale = jnp.exp(jax.random.uniform(key_columns, (1, 1, D), jnp.float32, math.log(0.3), math.log(3.0)))
    return (base * row_scale * column_scale).astype(jnp.bfloat16)


def steps_of(own_key, extent, cuts, smallest, largest):
    factor_of = 1.0
    for dim, blocks in cuts:
        steps = jax.random.uniform(jax.random.fold_in(jax.random.fold_in(own_key, 6), dim), (blocks,), jnp.float32, smallest / len(cuts), largest / len(cuts))
        factor_of = factor_of * jnp.repeat(jnp.exp(steps), extent[dim] // blocks).reshape((-1,) + (1,) * (len(extent) - 1 - dim))
    return factor_of


def scatter_about(rng, extent, deviation, most, cuts=(), kind=jnp.bfloat16):
    array = deviation * jax.random.normal(rng, extent, jnp.float32)
    if cuts:
        array = array * steps_of(rng, extent, cuts, -0.22, 0.18)
    return jnp.clip(array, -most, most).astype(kind)


def setup_inputs(seed: int = 0) -> dict:
    arg_keys = jax.random.split(jax.random.key(seed), 8)
    return {
        "states": draw_states(jax.random.fold_in(arg_keys[7], 71), 0),
        "cotangent": scatter_about(arg_keys[1], (ROLLOUTS, SEQ, KV), 1.0, 6.0, ((0, 32),)),
        "kv_weight": scatter_about(arg_keys[2], (D, KV), D ** -0.5, 0.125, ((0, 8),)),
        "norm_gain": scatter_about(arg_keys[3], (D,), 0.3, 1.5, ((0, 8),)),
        "prompt_len": draw_prompt_len(jax.random.fold_in(arg_keys[7], 71), 0),
        "response_len": draw_response_len(jax.random.fold_in(arg_keys[7], 71), 0),
        "reward_bucket": draw_reward_bucket(jax.random.fold_in(arg_keys[7], 71), 0),
    }


EPSILON = 1e-06

def reference(states, cotangent, kv_weight, norm_gain, prompt_len, response_len, reward_bucket):
    rollout_count = states.shape[0]
    seq_rows = states.shape[1]
    width = states.shape[2]
    feature_count = kv_weight.shape[1]
    reward_value = reward_bucket.astype(jnp.float32)
    token_total = jnp.sum(response_len.astype(jnp.float32))
    average = jnp.sum(reward_value) / rollout_count
    variance = jnp.sum(reward_value * reward_value) / rollout_count - average * average
    grad_scale = lax.rsqrt(variance + EPSILON) * lax.rsqrt(token_total)
    gain_wide = norm_gain.astype(jnp.float32)
    position = jnp.arange(seq_rows, dtype=jnp.int32)
    group_size = math.gcd(rollout_count, 64)
    group_count = rollout_count // group_size

    def one_group(totals, pieces):
        grad_weight, grad_gain = totals
        part_states, part_cotangent, part_prompt, part_response, part_reward = pieces
        widened = part_states.astype(jnp.float32)
        unit_rows = widened * lax.rsqrt(lax.optimization_barrier(jnp.mean(widened * widened, axis=-1, keepdims=True)) + EPSILON)
        normed = (unit_rows * (1.0 + gain_wide)).astype(jnp.bfloat16)
        flat_normed = normed.reshape(-1, width)
        key_values = jnp.dot(flat_normed, kv_weight, preferred_element_type=jnp.float32).astype(jnp.bfloat16)
        live_flag = (position[None, :] >= part_prompt[:, None]) & (position[None, :] < part_prompt[:, None] + part_response[:, None])
        coefficient = live_flag.astype(jnp.float32) * (part_reward - average)[:, None] * grad_scale
        weighted = (coefficient[:, :, None] * part_cotangent.astype(jnp.float32)).astype(jnp.bfloat16)
        flat_weighted = weighted.reshape(-1, feature_count)
        grad_weight = grad_weight + jnp.dot(flat_normed.T, flat_weighted, preferred_element_type=jnp.float32)
        backward = jnp.dot(flat_weighted, kv_weight.T, preferred_element_type=jnp.float32)
        grad_gain = grad_gain + lax.optimization_barrier(jnp.sum(unit_rows.reshape(-1, width) * backward, axis=0))
        return ((grad_weight, grad_gain), key_values.reshape(group_size, seq_rows, feature_count))
    start_totals = (jnp.zeros((width, feature_count), jnp.float32), jnp.zeros((width,), jnp.float32))
    grouped = (states.reshape(group_count, group_size, seq_rows, width), cotangent.reshape(group_count, group_size, seq_rows, feature_count), prompt_len.reshape(group_count, group_size), response_len.reshape(group_count, group_size), reward_value.reshape(group_count, group_size))
    (grad_weight, grad_gain), key_values = lax.scan(one_group, start_totals, grouped)
    return (key_values.reshape(rollout_count, seq_rows, feature_count), grad_weight, grad_gain)
```

```python
import functools

import jax
import jax.numpy as jnp
from jax import lax
from jax.experimental import pallas as pl
from jax.experimental.pallas import tpu as pltpu
from jax.sharding import PartitionSpec as P

EPSILON = 1e-06
MESH = pl.DeviceIdType.MESH
BF = jnp.bfloat16
F32 = jnp.float32
TILE = 256
HOP = 8


def flip(me, mask):
    out = me
    bit = 0
    while mask >> bit:
        if (mask >> bit) & 1:
            own = lax.rem(lax.div(me, 1 << bit), 2)
            out = out + (1 - 2 * own) * (1 << bit)
        bit += 1
    return out


def offset_of(position, order):
    count = len(order)
    return sum(((position >> (count - 1 - i)) & 1) << order[i] for i in range(count))


def plan(R, F):
    bits = F.bit_length() - 2
    count = 1 << bits
    everyone = [(k, m) for k in range(R) for m in range(count) if k or m]
    if R * count <= 32:
        stages = [everyone]
    else:
        stages = [[e for e in everyone if not e[0]], [e for e in everyone if not e[1]]]
    return bits, count, stages


def kernel(
    R, F, chunk_rows,
    states_hbm, cot_hbm, weight_hbm, gain_hbm, prompt_ref, response_ref, reward_ref,
    kv_ref, gw_ref, gg_ref,
    states, cot, scaled, weight, w_all, gain,
    grad, grad_send, grad_in, sending, receiving, own, chain_out, chain_in,
    fin_out, fin_in, scal_out, scal_pair, scal_in, acc, inverse, gcol, wide_gain,
    load_sem, w_send, w_recv, fw_send, fw_recv, g_send, g_recv, x_send, x_recv,
    z_send, z_recv, fin_send, fin_recv, s_send, s_recv, gate,
):
    r, f = lax.axis_index("replica"), lax.axis_index("fsdp")
    bits, count, stages = plan(R, F)
    orders = (list(range(bits)), list(range(bits))[::-1])
    j = lax.div(f, 2)
    odd = lax.rem(f, 2) == 1
    seq, width = states.shape
    features = cot.shape[1]
    half = features // 2
    rows = weight.shape[0]
    pair = 2 * rows
    tiles = width // TILE
    chunks = pair // chunk_rows
    partner = (r, flip(f, 1))
    pending = []

    def remote(src, dst, send_sem, recv_sem, device):
        return pltpu.make_async_remote_copy(
            src_ref=src, dst_ref=dst, send_sem=send_sem, recv_sem=recv_sem,
            device_id=device, device_id_type=MESH,
        )

    def launch(copy):
        copy.start()
        pending.append(copy)
        return copy

    def finish():
        for copy in pending:
            copy.wait_send()
        pending.clear()

    def across(bit):
        return (r, flip(f, 2 << bit))

    def peer(k, m):
        return (lax.rem(r + k, R), flip(f, m << 1))

    def pair_begin(m):
        return pl.multiple_of(flip(j, m) * pair, pair)

    loads = [
        pltpu.make_async_copy(src, dst, load_sem.at[i])
        for i, (src, dst) in enumerate([
            (gain_hbm, gain), (weight_hbm, weight), (states_hbm.at[0], states), (cot_hbm.at[0], cot),
        ])
    ]
    for copy in loads:
        copy.start()
    gain_load, weight_load, states_load, cot_load = loads

    barrier = pltpu.get_barrier_semaphore()
    pl.semaphore_signal(barrier, inc=1, device_id=partner, device_id_type=MESH)
    peers = [e for stage in stages for e in stage]

    @pl.when(odd)
    def _():
        for k, m in peers:
            pl.semaphore_signal(barrier, inc=1, device_id=peer(k, m), device_id_type=MESH)

    @pl.when(jnp.logical_not(odd))
    def _():
        for bit in range(bits):
            pl.semaphore_signal(barrier, inc=1, device_id=across(bit), device_id_type=MESH)

    lane = lax.broadcasted_iota(jnp.int32, (1, 128), 1)
    diagonal = lax.broadcasted_iota(jnp.int32, (rows, rows), 0) == lax.broadcasted_iota(
        jnp.int32, (rows, rows), 1
    )
    mine = pl.multiple_of(f * rows, rows)

    def scalars():
        reward = reward_ref[0].astype(F32)
        tokens = response_ref[0].astype(F32)
        zero = jnp.zeros((1, 128), F32)
        out = jnp.where(lane == 0, zero + reward, zero)
        out = jnp.where(lane == 1, zero + reward * reward, out)
        return jnp.where(lane == 2, zero + tokens, out), reward

    def scale_weight():
        gain_load.wait()
        row = gain[...].astype(F32).reshape(1, rows) + 1.0
        column = jnp.sum(jnp.where(diagonal, row, 0.0), axis=1, keepdims=True)
        wide_gain[...] = jnp.broadcast_to(column, wide_gain.shape)
        weight_load.wait()
        w_all[pl.ds(mine, rows), :] = (weight[...].astype(F32) * column).astype(BF)

    def scale_cotangent():
        states_load.wait()

        def square_tile(i, total):
            at = pl.multiple_of(i * TILE, TILE)
            for k in range(0, TILE, 128):
                part = states[:, pl.ds(at + k, 128)].astype(F32)
                total = total + part * part
            return total

        squares = lax.fori_loop(0, tiles, square_tile, jnp.zeros((seq, 128), F32))
        inverse[...] = lax.rsqrt(jnp.sum(squares, axis=1, keepdims=True) / width + EPSILON)
        cot_load.wait()
        position = lax.broadcasted_iota(jnp.int32, (seq, features), 0)
        first = prompt_ref[0]
        alive = (position >= first) & (position < first + response_ref[0])
        scaled[...] = jnp.where(alive, cot[...].astype(F32) * inverse[...], 0.0).astype(BF)

    def gradient(target, after):
        def tile(begin):
            at = pl.ds(pl.multiple_of(begin, TILE), TILE)
            target[at, :] = lax.dot_general(
                states[:, at], scaled[...], (((0,), (0,)), ((), ())), preferred_element_type=F32
            ).astype(target.dtype)

        def natural(i, carry):
            tile(i * TILE)
            return carry

        aligned = rows % TILE == 0
        if not aligned:
            lax.fori_loop(0, tiles, natural, 0)
        for h in range(2):
            for m in reversed(range(count)):
                begin = pair_begin(m) + h * rows
                if aligned:
                    for k in range(0, rows, TILE):
                        tile(begin + k)
                after(m, h, pl.multiple_of(begin, rows))

    def product(m, start):
        if pair % 128:
            return
        at = pl.ds(pair_begin(m), pair)
        value = jnp.dot(states[:, at], w_all[at, :], preferred_element_type=F32)
        acc[...] = value if start else acc[...] + value

    def key_values():
        if pair % 128:
            acc[...] = jnp.dot(states[...], w_all[...], preferred_element_type=F32)
        kv_ref[0] = jnp.where(inverse[...] > 0.0, acc[...] * inverse[...], 0.0).astype(BF)

    def last(order, m):
        return max(i for i in range(bits) if (m >> order[i]) & 1)

    def w_copy(p, m, h):
        bit = orders[p][last(orders[p], m)]
        at = pl.ds(pl.multiple_of(pair_begin(m ^ (1 << bit)) + h * rows, rows), rows)
        ref = w_all.at[at, pl.ds(p * half, half)]
        i = (p * count + m) * 2 + h
        return remote(ref, ref, w_send.at[i], w_recv.at[i], across(bit))

    def fw_copy(p, m, h):
        at = pl.ds(pl.multiple_of(pair_begin(m) + h * rows, rows), rows)
        ref = w_all.at[at, pl.ds(p * half, half)]
        i = (p * count + m) * 2 + h
        return remote(ref, ref, fw_send.at[i], fw_recv.at[i], partner)

    def odd_copy():
        at = pl.ds(pl.multiple_of(j * pair + rows, rows), rows)
        ref = w_all.at[at, :]
        return remote(ref, ref, fw_send.at[1], fw_recv.at[1], partner)

    def g_copy(m, h, begin):
        i = m * 2 + h
        return remote(
            grad_send.at[pl.ds(begin, rows)], grad_in.at[m, pl.ds(h * rows, rows)],
            g_send.at[i], g_recv.at[i], partner,
        )

    def fin_copy(c):
        return remote(fin_out.at[c], fin_in.at[c], fin_send.at[c], fin_recv.at[c], partner)

    def pair_scalars():
        return remote(scal_pair.at[0], scal_pair.at[1], s_send.at[0], s_recv.at[0], partner)

    def finished(total, c):
        at = slice((c % (chunks // 2)) * chunk_rows, (c % (chunks // 2) + 1) * chunk_rows)
        column = wide_gain[at, 0:1]
        gw_ref[at, :] = total * column
        gcol[at, :] = jnp.sum(total * weight[at, :].astype(F32), axis=1, keepdims=True)

    def grad_gain():
        gg_ref[...] = jnp.sum(jnp.where(diagonal, gcol[...], 0.0), axis=0, keepdims=True)

    levels = [[m for m in range(count) if m.bit_count() == n] for n in range(bits + 1)]

    @pl.when(jnp.logical_not(odd))
    def _():
        pl.semaphore_wait(barrier, bits + 1)
        scal, _ = scalars()
        scal_pair[0] = scal
        launch(pair_scalars())
        scale_weight()
        for s in range(bits):
            for p in range(2):
                launch(w_copy(p, 1 << orders[p][s], 0))
        scale_cotangent()
        gradient(grad_send, lambda m, h, begin: launch(g_copy(m, h, begin)))
        odd_copy().wait_recv()
        for s in range(bits):
            for p in range(2):
                launch(w_copy(p, 1 << orders[p][s], 1))
        for p in range(2):
            launch(fw_copy(p, 0, 0))
        product(0, True)
        for n in range(1, bits + 1):
            for m in levels[n]:
                for p in range(2):
                    for h in range(2):
                        w_copy(p, m, h).wait_recv()
                        launch(fw_copy(p, m, h))
            if n == 1:
                pl.semaphore_wait(gate, 1)
            for m in levels[n]:
                for p in range(2):
                    for s in range(last(orders[p], m) + 1, bits):
                        for h in range(2):
                            launch(w_copy(p, m | (1 << orders[p][s]), h))
            for m in levels[n]:
                product(m, False)
        key_values()
        for c in range(chunks // 2):
            fin_copy(c).wait_recv()
            finished(fin_in[c], c)
        grad_gain()
        finish()

    @pl.when(odd)
    def _():
        pl.semaphore_wait(barrier, len(peers) + 1)
        scal, reward = scalars()
        pair_scalars().wait_recv()
        low = scal_pair[1]
        total = scal + low
        slot = 0

        def exchange(stage, slot):
            copies = []
            for k, m in stage:
                copies.append(launch(remote(
                    scal_out.at[which], scal_in.at[slot], s_send.at[1 + slot], s_recv.at[1 + slot],
                    peer(k, m),
                )))
                slot += 1
            return copies, slot

        def collect(total, copies, slot):
            for copy in copies:
                copy.wait_recv()
            for i in range(slot - len(copies), slot):
                total = total + scal_in[i]
            return total

        which = 0
        scal_out[0] = total
        copies, slot = exchange(stages[0], slot)
        scale_weight()
        launch(odd_copy())
        scale_cotangent()
        gradient(grad, lambda m, h, begin: None)
        total = collect(total, copies, slot)
        for which in range(1, len(stages)):
            scal_out[which] = total
            copies, slot = exchange(stages[which], slot)
            total = collect(total, copies, slot)

        def pick(source, index):
            return jnp.sum(jnp.where(lane == index, source, 0.0), axis=1, keepdims=True)

        number = float(R * F)
        average = pick(total, 0) / number
        variance = pick(total, 1) / number - average * average
        size = lax.rsqrt(variance + EPSILON) * lax.rsqrt(pick(total, 2))
        coef = (reward - average) * size
        coef_low = (pick(low, 0) - average) * size

        starts = [count - (count >> i) for i in range(bits + 1)]
        arrived = set()

        def chunk_at(c):
            return pl.ds(c * chunk_rows, chunk_rows)

        def partial(p, q, c, step):
            m = offset_of(q, orders[p])
            h = c // (chunks // 2)
            if (m, h) not in arrived:
                arrived.add((m, h))
                g_copy(m, h, pl.multiple_of(pair_begin(m) + h * rows, rows)).wait_recv()
            columns = slice(p * half, (p + 1) * half)
            begin = pl.multiple_of(pair_begin(m) + c * chunk_rows, chunk_rows)
            value = grad[pl.ds(begin, chunk_rows), columns] * coef
            value = value + grad_in[m, chunk_at(c), columns].astype(F32) * coef_low
            for i in range(step):
                x_copy(p, i, q, c).wait_recv()
                value = value + receiving[p, starts[i] + q, chunk_at(c)].astype(F32)
            return value

        def x_copy(p, step, q, c):
            i = (p * (count - 1) + starts[step] + q) * chunks + c
            return remote(
                sending.at[p, starts[step] + q, chunk_at(c)],
                receiving.at[p, starts[step] + q, chunk_at(c)],
                x_send.at[i], x_recv.at[i], across(orders[p][step]),
            )

        def scatter(step, q, c):
            keep = count >> (step + 1)
            for p in range(2):
                sending[p, starts[step] + q, chunk_at(c)] = partial(p, keep + q, c, step).astype(BF)
                launch(x_copy(p, step, q, c))

        def z_copy(way, c):
            after = r + 1 - 2 * way
            return remote(
                chain_out.at[way, c], chain_in.at[way, c],
                z_send.at[way * chunks + c], z_recv.at[way * chunks + c],
                (lax.rem(after + R, R), f),
            )

        def place(way):
            return r if way == 0 else R - 1 - r

        def gather_own(c):
            for p in range(2):
                own[c, :, p * half:(p + 1) * half] = partial(p, 0, c, bits)

        def relay(hop, c):
            for way in range(2):
                @pl.when(place(way) == hop)
                def _(way=way):
                    value = own[c]
                    if hop:
                        z_copy(way, c).wait_recv()
                        value = value + chain_in[way, c].astype(F32)
                    chain_out[way, c] = value.astype(chain_out.dtype)
                    z_copy(way, c).start()

        def total_of(c):
            for way in range(2):
                @pl.when(place(way) == R - 1)
                def _(way=way):
                    z_copy(way, c).wait_recv()
            value = own[c]
            for way in range(2):
                value = value + jnp.where(place(way) > 0, chain_in[way, c].astype(F32), 0.0)
            if c < chunks // 2:
                fin_out[c] = value
                launch(fin_copy(c))
            else:
                finished(value, c)

        def products(n):
            for m in levels[n]:
                for p in range(2):
                    for h in range(2 if m else 1):
                        fw_copy(p, m, h).wait_recv()
                product(m, m == 0)

        def open_gate():
            pl.semaphore_signal(gate, inc=1, device_id=partner, device_id_type=MESH)

        events = []

        def at(key, action, *arguments):
            events.append((key, len(events), action, arguments))

        period = count - 1
        final = HOP * bits
        for c in range(chunks):
            for step in range(bits):
                keep = count >> (step + 1)
                for q in reversed(range(keep)):
                    late = 0 if 2 * q >= keep and keep > 1 else HOP - 2
                    if step == bits - 1:
                        late = 0
                    at(period * c + HOP * step + late, scatter, step, q, c)
            at(period * c + final, gather_own, c)
            for hop in range(R - 1):
                at(period * c + final + HOP * hop, relay, hop, c)
            at(period * c + final + HOP * (R - 1), total_of, c)
        ending = period * (chunks - 1) + final
        at(ending - HOP // 2, open_gate)
        at(ending - HOP, products, 0)
        for n in range(1, bits + 1):
            at(ending + n if n < bits else ending + HOP * (R - 2) + 1, products, n)
        at(ending + HOP * (R - 2) + 2, key_values)
        for _, _, action, arguments in sorted(events, key=lambda e: e[:2]):
            action(*arguments)
        grad_gain()
        finish()
        for way in range(2):
            @pl.when(place(way) < R - 1)
            def _(way=way):
                for c in range(chunks):
                    z_copy(way, c).wait_send()


def shards(R, F, states, cotangent, kv_weight, norm_gain, prompt_len, response_len, reward_bucket):
    _, seq, width = states.shape
    rows, features = kv_weight.shape
    half = features // 2
    bits, count, stages = plan(R, F)
    pair = 2 * rows
    chunk_rows = max(pair // 8, 16)
    chunks = pair // chunk_rows
    wire = BF if R <= 4 else F32
    slots = sum(len(stage) for stage in stages)
    vmem = pl.BlockSpec(memory_space=pltpu.VMEM)
    hbm = pl.BlockSpec(memory_space=pltpu.HBM)
    smem = pl.BlockSpec(memory_space=pltpu.SMEM)
    dma = pltpu.SemaphoreType.DMA
    key_values, grad_weight, grad_gain = pl.pallas_call(
        functools.partial(kernel, R, F, chunk_rows),
        out_shape=(
            jax.ShapeDtypeStruct((1, seq, features), BF),
            jax.ShapeDtypeStruct((rows, features), F32),
            jax.ShapeDtypeStruct((1, rows), F32),
        ),
        in_specs=[hbm] * 4 + [smem] * 3,
        out_specs=(vmem, vmem, vmem),
        scratch_shapes=[
            pltpu.VMEM((seq, width), BF),
            pltpu.VMEM((seq, features), BF),
            pltpu.VMEM((seq, features), BF),
            pltpu.VMEM((rows, features), BF),
            pltpu.VMEM((width, features), BF),
            pltpu.VMEM((rows,), BF),
            pltpu.VMEM((width, features), F32),
            pltpu.VMEM((width, features), BF),
            pltpu.VMEM((count, pair, features), BF),
            pltpu.VMEM((2, max(count - 1, 1), pair, half), BF),
            pltpu.VMEM((2, max(count - 1, 1), pair, half), BF),
            pltpu.VMEM((chunks, chunk_rows, features), F32),
            pltpu.VMEM((2, chunks, chunk_rows, features), wire),
            pltpu.VMEM((2, chunks, chunk_rows, features), wire),
            pltpu.VMEM((chunks // 2, chunk_rows, features), F32),
            pltpu.VMEM((chunks // 2, chunk_rows, features), F32),
            pltpu.VMEM((len(stages), 1, 128), F32),
            pltpu.VMEM((2, 1, 128), F32),
            pltpu.VMEM((slots, 1, 128), F32),
            pltpu.VMEM((seq, features), F32),
            pltpu.VMEM((seq, 1), F32),
            pltpu.VMEM((rows, 1), F32),
            pltpu.VMEM((rows, 128), F32),
            dma((4,)),
            dma((4 * count,)), dma((4 * count,)),
            dma((4 * count,)), dma((4 * count,)),
            dma((2 * count,)), dma((2 * count,)),
            dma((2 * count * chunks,)), dma((2 * count * chunks,)),
            dma((2 * chunks,)), dma((2 * chunks,)),
            dma((chunks // 2,)), dma((chunks // 2,)),
            dma((1 + slots,)), dma((1 + slots,)),
            pltpu.SemaphoreType.REGULAR,
        ],
        compiler_params=pltpu.CompilerParams(
            collective_id=0, has_side_effects=True, vmem_limit_bytes=40 * 1024 * 1024
        ),
    )(
        *[
            pltpu.with_memory_space_constraint(x, pltpu.HBM)
            for x in (states, cotangent, kv_weight, norm_gain)
        ],
        prompt_len, response_len, reward_bucket,
    )
    return key_values, grad_weight, grad_gain.reshape(rows)


def solution(mesh):
    placed = (
        P(("replica", "fsdp"), None, None),
        P(("replica", "fsdp"), None, None),
        P("fsdp", None),
        P("fsdp"),
        P(("replica", "fsdp")),
        P(("replica", "fsdp")),
        P(("replica", "fsdp")),
    )
    return jax.shard_map(
        functools.partial(shards, mesh.shape["replica"], mesh.shape["fsdp"]),
        mesh=mesh,
        in_specs=placed,
        out_specs=(P(("replica", "fsdp"), None, None), P("fsdp", None), P("fsdp")),
        check_vma=False,
    )
```

```python
import functools

import jax
import jax.numpy as jnp
from jax import lax
from jax.experimental import pallas as pl
from jax.experimental.pallas import tpu as pltpu
from jax.sharding import PartitionSpec as P

EPSILON = 1e-06
MESH = pl.DeviceIdType.MESH
BF = jnp.bfloat16
F32 = jnp.float32
TILE = 256
LAG = 11
HOP = 8


def flip(me, mask):
    out = me
    bit = 0
    while mask >> bit:
        if (mask >> bit) & 1:
            own = lax.rem(lax.div(me, 1 << bit), 2)
            out = out + (1 - 2 * own) * (1 << bit)
        bit += 1
    return out


def offset_of(position, order):
    count = len(order)
    return sum(((position >> (count - 1 - i)) & 1) << order[i] for i in range(count))


def plan(R, F):
    bits = F.bit_length() - 2
    count = 1 << bits
    everyone = [(k, m) for k in range(R) for m in range(count) if k or m]
    if R * count <= 32:
        stages = [everyone]
    else:
        stages = [[e for e in everyone if not e[0]], [e for e in everyone if not e[1]]]
    return bits, count, stages


def kernel(
    R, F, chunk_rows,
    states_hbm, cot_hbm, weight_hbm, gain_hbm, prompt_ref, response_ref, reward_ref,
    kv_ref, gw_ref, gg_ref,
    states, cot, scaled, weight, w_all, gain,
    grad, grad_send, grad_in, sending, receiving, own, chain_out, chain_in,
    fin_out, fin_in, scal_out, scal_pair, scal_in, acc, inverse, gcol, wide_gain,
    load_sem, send_sem, w_recv, fw_recv, g_recv, x_recv, z_recv, fin_recv, s_recv, gate,
):
    r, f = lax.axis_index("replica"), lax.axis_index("fsdp")
    bits, count, stages = plan(R, F)
    orders = (list(range(bits)), list(range(bits))[::-1])
    j = lax.div(f, 2)
    odd = lax.rem(f, 2) == 1
    seq, width = states.shape
    features = cot.shape[1]
    half = features // 2
    rows = weight.shape[0]
    pair = 2 * rows
    tiles = width // TILE
    chunks = pair // chunk_rows
    partner = (r, flip(f, 1))

    def remote(src, dst, send_sem, recv_sem, device):
        return pltpu.make_async_remote_copy(
            src_ref=src, dst_ref=dst, send_sem=send_sem, recv_sem=recv_sem,
            device_id=device, device_id_type=MESH,
        )

    def sent(ref, send_sem):
        remote(ref, ref, send_sem, send_sem, partner).wait_send()

    def got(ref, recv_sem):
        remote(ref, ref, recv_sem, recv_sem, partner).wait_recv()

    def across(bit):
        return (r, flip(f, 2 << bit))

    def peer(k, m):
        return (lax.rem(r + k, R), flip(f, m << 1))

    def pair_begin(m):
        return pl.multiple_of(flip(j, m) * pair, pair)

    loads = [
        pltpu.make_async_copy(src, dst, load_sem.at[i])
        for i, (src, dst) in enumerate([
            (gain_hbm, gain), (weight_hbm, weight), (states_hbm.at[0], states), (cot_hbm.at[0], cot),
        ])
    ]
    for copy in loads:
        copy.start()
    gain_load, weight_load, states_load, cot_load = loads

    barrier = pltpu.get_barrier_semaphore()
    pl.semaphore_signal(barrier, inc=1, device_id=partner, device_id_type=MESH)
    peers = [e for stage in stages for e in stage]

    @pl.when(odd)
    def _():
        for k, m in peers:
            pl.semaphore_signal(barrier, inc=1, device_id=peer(k, m), device_id_type=MESH)

    @pl.when(jnp.logical_not(odd))
    def _():
        for bit in range(bits):
            pl.semaphore_signal(barrier, inc=1, device_id=across(bit), device_id_type=MESH)

    lane = lax.broadcasted_iota(jnp.int32, (1, 128), 1)
    diagonal = lax.broadcasted_iota(jnp.int32, (rows, rows), 0) == lax.broadcasted_iota(
        jnp.int32, (rows, rows), 1
    )
    mine = pl.multiple_of(f * rows, rows)

    def scalars():
        reward = reward_ref[0].astype(F32)
        tokens = response_ref[0].astype(F32)
        zero = jnp.zeros((1, 128), F32)
        out = jnp.where(lane == 0, zero + reward, zero)
        out = jnp.where(lane == 1, zero + reward * reward, out)
        return jnp.where(lane == 2, zero + tokens, out), reward

    def scale_weight():
        gain_load.wait()
        row = gain[...].astype(F32).reshape(1, rows) + 1.0
        column = jnp.sum(jnp.where(diagonal, row, 0.0), axis=1, keepdims=True)
        wide_gain[...] = jnp.broadcast_to(column, wide_gain.shape)
        weight_load.wait()
        w_all[pl.ds(mine, rows), :] = (weight[...].astype(F32) * column).astype(BF)

    def scale_cotangent():
        states_load.wait()

        def square_tile(i, total):
            at = pl.multiple_of(i * TILE, TILE)
            for k in range(0, TILE, 128):
                part = states[:, pl.ds(at + k, 128)].astype(F32)
                total = total + part * part
            return total

        squares = lax.fori_loop(0, tiles, square_tile, jnp.zeros((seq, 128), F32))
        inverse[...] = lax.rsqrt(jnp.sum(squares, axis=1, keepdims=True) / width + EPSILON)
        cot_load.wait()
        position = lax.broadcasted_iota(jnp.int32, (seq, features), 0)
        first = prompt_ref[0]
        alive = (position >= first) & (position < first + response_ref[0])
        scaled[...] = jnp.where(alive, cot[...].astype(F32) * inverse[...], 0.0).astype(BF)

    def gradient(target, after):
        def tile(begin):
            at = pl.ds(pl.multiple_of(begin, TILE), TILE)
            target[at, :] = lax.dot_general(
                states[:, at], scaled[...], (((0,), (0,)), ((), ())), preferred_element_type=F32
            ).astype(target.dtype)

        def natural(i, carry):
            tile(i * TILE)
            return carry

        aligned = rows % TILE == 0
        if not aligned:
            lax.fori_loop(0, tiles, natural, 0)
        for h in range(2):
            for m in reversed(range(count)):
                begin = pair_begin(m) + h * rows
                if aligned:
                    for k in range(0, rows, TILE):
                        tile(begin + k)
                after(m, h, pl.multiple_of(begin, rows))

    def product(m, start):
        if pair % 128:
            return
        at = pl.ds(pair_begin(m), pair)
        value = jnp.dot(states[:, at], w_all[at, :], preferred_element_type=F32)
        acc[...] = value if start else acc[...] + value

    def key_values():
        if pair % 128:
            acc[...] = jnp.dot(states[...], w_all[...], preferred_element_type=F32)
        kv_ref[0] = jnp.where(inverse[...] > 0.0, acc[...] * inverse[...], 0.0).astype(BF)

    def last(order, m):
        return max(i for i in range(bits) if (m >> order[i]) & 1)

    def w_rows(m, h):
        return pl.ds(pl.multiple_of(pair_begin(m) + h * rows, rows), rows)

    def w_copy(p, m, h):
        bit = orders[p][last(orders[p], m)]
        ref = w_all.at[w_rows(m ^ (1 << bit), h), pl.ds(p * half, half)]
        return remote(ref, ref, send_sem.at[0], w_recv.at[p * count + m], across(bit))

    def hand(p, m, h):
        ref = w_all.at[w_rows(m, h), pl.ds(p * half, half)]
        remote(ref, ref, send_sem.at[1], fw_recv.at[m], partner).start()

    def handed(m, h):
        got(w_all.at[w_rows(m, h)], fw_recv.at[m])

    def received(p, m, h):
        w_copy(p, m, h).wait_recv()
        hand(p, m, h)

    def forward(p, m, h):
        for s in range(last(orders[p], m) + 1, bits):
            w_copy(p, m | (1 << orders[p][s]), h).start()

    def g_copy(m, h, begin):
        return remote(
            grad_send.at[pl.ds(begin, rows)], grad_in.at[m, pl.ds(h * rows, rows)],
            send_sem.at[2], g_recv.at[m * 2 + h], partner,
        )

    def fin_copy(c):
        return remote(fin_out.at[c], fin_in.at[c], send_sem.at[2], fin_recv.at[c], partner)

    def pair_scalars():
        return remote(scal_pair.at[0], scal_pair.at[1], send_sem.at[3], s_recv.at[0], partner)

    def finish_weight():
        sent(w_all.at[pl.ds(0, (count - 1) * rows)], send_sem.at[0])
        sent(w_all.at[pl.ds(0, count * rows)], send_sem.at[1])

    def finished(total, c):
        at = slice((c % (chunks // 2)) * chunk_rows, (c % (chunks // 2) + 1) * chunk_rows)
        column = wide_gain[at, 0:1]
        gw_ref[at, :] = total * column
        gcol[at, :] = jnp.sum(total * weight[at, :].astype(F32), axis=1, keepdims=True)

    def grad_gain():
        gg_ref[...] = jnp.sum(jnp.where(diagonal, gcol[...], 0.0), axis=0, keepdims=True)

    levels = [[m for m in range(count) if m.bit_count() == n] for n in range(bits + 1)]
    firsts = [(p, 1 << orders[p][0]) for p in range(2)]

    @pl.when(jnp.logical_not(odd))
    def _():
        pl.semaphore_wait(barrier, bits + 1)
        scal, _ = scalars()
        scal_pair[0] = scal
        pair_scalars().start()
        scale_weight()
        for s in range(bits):
            for p in range(2):
                w_copy(p, 1 << orders[p][s], 0).start()
        scale_cotangent()
        gradient(grad_send, lambda m, h, begin: g_copy(m, h, begin).start())
        for p in range(2):
            hand(p, 0, 0)
        handed(0, 1)
        product(0, True)
        for m in levels[1]:
            for p in range(2):
                received(p, m, 0)
        pl.semaphore_wait(gate, 1)
        for n in range(1, bits + 1):
            for m in levels[n]:
                for p in range(2):
                    if n > 1:
                        received(p, m, 0)
                    forward(p, m, 0)
        for n in range(1, bits + 1):
            for m in levels[n]:
                handed(m, 1)
                product(m, False)
        key_values()
        for c in range(chunks // 2):
            fin_copy(c).wait_recv()
            finished(fin_in[c], c)
        grad_gain()
        finish_weight()
        sent(grad_send, send_sem.at[2])
        sent(scal_pair.at[0], send_sem.at[3])

    @pl.when(odd)
    def _():
        pl.semaphore_wait(barrier, len(peers) + 1)
        scal, reward = scalars()
        pair_scalars().wait_recv()
        low = scal_pair[1]
        total = scal + low

        def exchange(which, total):
            first = sum(len(stage) for stage in stages[:which])
            scal_out[which] = total
            for i, (k, m) in enumerate(stages[which]):
                remote(
                    scal_out.at[which], scal_in.at[first + i], send_sem.at[3],
                    s_recv.at[1 + which], peer(k, m),
                ).start()

        def collect(which, total):
            first = sum(len(stage) for stage in stages[:which])
            size = len(stages[which])
            got(scal_in.at[pl.ds(first, size)], s_recv.at[1 + which])
            for i in range(first, first + size):
                total = total + scal_in[i]
            return total

        exchange(0, total)
        scale_weight()
        for p, m in firsts:
            w_copy(p, m, 1).start()
        for p in range(2):
            hand(p, 0, 1)
        scale_cotangent()
        gradient(grad, lambda m, h, begin: None)
        total = collect(0, total)
        for which in range(1, len(stages)):
            exchange(which, total)
            total = collect(which, total)

        def pick(source, index):
            return jnp.sum(jnp.where(lane == index, source, 0.0), axis=1, keepdims=True)

        number = float(R * F)
        average = pick(total, 0) / number
        variance = pick(total, 1) / number - average * average
        size = lax.rsqrt(variance + EPSILON) * lax.rsqrt(pick(total, 2))
        coef = (reward - average) * size
        coef_low = (pick(low, 0) - average) * size

        starts = [count - (count >> i) for i in range(bits + 1)]
        arrived = set()

        def chunk_at(c):
            return pl.ds(c * chunk_rows, chunk_rows)

        def arrive(q, c, step):
            for p in range(2):
                m, h = offset_of(q, orders[p]), c // (chunks // 2)
                if (m, h) not in arrived:
                    arrived.add((m, h))
                    g_copy(m, h, w_rows(m, h).start).wait_recv()
            for i in range(step):
                slot = starts[i] + q
                got(receiving.at[:, slot, chunk_at(c)], x_recv.at[slot * chunks + c])

        def partial(p, q, c, step):
            m = offset_of(q, orders[p])
            columns = slice(p * half, (p + 1) * half)
            begin = pl.multiple_of(pair_begin(m) + c * chunk_rows, chunk_rows)
            value = grad[pl.ds(begin, chunk_rows), columns] * coef
            value = value + grad_in[m, chunk_at(c), columns].astype(F32) * coef_low
            for i in range(step):
                value = value + receiving[p, starts[i] + q, chunk_at(c)].astype(F32)
            return value

        def scatter(step, q, c):
            keep = count >> (step + 1)
            slot = starts[step] + q
            arrive(keep + q, c, step)
            for p in range(2):
                sending[p, slot, chunk_at(c)] = partial(p, keep + q, c, step).astype(BF)
                remote(
                    sending.at[p, slot, chunk_at(c)], receiving.at[p, slot, chunk_at(c)],
                    send_sem.at[4], x_recv.at[slot * chunks + c], across(orders[p][step]),
                ).start()

        def z_copy(way, c, p):
            after = r + 1 - 2 * way
            columns = pl.ds(p * half, half)
            return remote(
                chain_out.at[way, c, :, columns], chain_in.at[way, c, :, columns],
                send_sem.at[5 + way], z_recv.at[(way * chunks + c) * 2 + p],
                (lax.rem(after + R, R), f),
            )

        def place(way):
            return r if way == 0 else R - 1 - r

        def gather_own(c):
            arrive(0, c, bits)
            for p in range(2):
                own[c, :, p * half:(p + 1) * half] = partial(p, 0, c, bits)

        def relay(hop, c):
            for way in range(2):
                @pl.when(place(way) == hop)
                def _(way=way):
                    for p in range(2):
                        columns = slice(p * half, (p + 1) * half)
                        value = own[c, :, columns]
                        if hop:
                            z_copy(way, c, p).wait_recv()
                            value = value + chain_in[way, c, :, columns].astype(F32)
                        chain_out[way, c, :, columns] = value.astype(chain_out.dtype)
                        z_copy(way, c, p).start()

        def total_of(c):
            for way in range(2):
                @pl.when(place(way) == R - 1)
                def _(way=way):
                    for p in range(2):
                        z_copy(way, c, p).wait_recv()
            value = own[c]
            for way in range(2):
                value = value + jnp.where(place(way) > 0, chain_in[way, c].astype(F32), 0.0)
            if c < chunks // 2:
                fin_out[c] = value
                fin_copy(c).start()
            else:
                finished(value, c)

        def products(n):
            for m in levels[n]:
                handed(m, 0)
                product(m, m == 0)

        def open_gate():
            pl.semaphore_signal(gate, inc=1, device_id=partner, device_id_type=MESH)

        def weight_first():
            for p, m in firsts:
                received(p, m, 1)

        def weight_second():
            for p, m in firsts:
                for s in range(1, bits):
                    w_copy(p, 1 << orders[p][s], 1).start()
                forward(p, m, 1)

        def weight_level(n):
            for m in levels[n]:
                for p in range(2):
                    if (p, m) not in firsts:
                        received(p, m, 1)
                        forward(p, m, 1)

        events = []

        def at(key, action, *arguments):
            events.append((key, len(events), action, arguments))

        period = count - 1
        final = LAG * bits
        for c in range(chunks):
            for step in range(bits):
                keep = count >> (step + 1)
                for q in reversed(range(keep)):
                    late = 6 if 2 * q < keep and step < bits - 1 else 0
                    at(period * c + LAG * step + late, scatter, step, q, c)
            at(period * c + final, gather_own, c)
            for hop in range(R - 1):
                at(period * c + final + HOP * hop, relay, hop, c)
            at(period * c + final + HOP * (R - 1), total_of, c)
        scattered = period * (chunks - 1) + LAG * (bits - 1)
        ending = period * (chunks - 1) + final + HOP * (R - 1)
        at(final, weight_first)
        at(final, products, 0)
        at(scattered, weight_second)
        at(scattered + 5, open_gate)
        for n in range(1, bits + 1):
            late = (bits - n) * HOP
            at(ending - 14 - late, weight_level, n)
            at(ending - 9 - late, products, n)
        at(ending - 9, key_values)
        for _, _, action, arguments in sorted(events, key=lambda e: e[:2]):
            action(*arguments)
        grad_gain()
        finish_weight()
        sent(fin_out, send_sem.at[2])
        sent(scal_in, send_sem.at[3])
        sent(sending, send_sem.at[4])
        for way in range(2):
            @pl.when(place(way) < R - 1)
            def _(way=way):
                sent(chain_out.at[way], send_sem.at[5 + way])


def shards(R, F, states, cotangent, kv_weight, norm_gain, prompt_len, response_len, reward_bucket):
    _, seq, width = states.shape
    rows, features = kv_weight.shape
    half = features // 2
    bits, count, stages = plan(R, F)
    pair = 2 * rows
    chunk_rows = max(pair // 8, 16)
    chunks = pair // chunk_rows
    wire = BF if R <= 4 else F32
    slots = sum(len(stage) for stage in stages)
    vmem = pl.BlockSpec(memory_space=pltpu.VMEM)
    hbm = pl.BlockSpec(memory_space=pltpu.HBM)
    smem = pl.BlockSpec(memory_space=pltpu.SMEM)
    dma = pltpu.SemaphoreType.DMA
    key_values, grad_weight, grad_gain = pl.pallas_call(
        functools.partial(kernel, R, F, chunk_rows),
        out_shape=(
            jax.ShapeDtypeStruct((1, seq, features), BF),
            jax.ShapeDtypeStruct((rows, features), F32),
            jax.ShapeDtypeStruct((1, rows), F32),
        ),
        in_specs=[hbm] * 4 + [smem] * 3,
        out_specs=(vmem, vmem, vmem),
        scratch_shapes=[
            pltpu.VMEM((seq, width), BF),
            pltpu.VMEM((seq, features), BF),
            pltpu.VMEM((seq, features), BF),
            pltpu.VMEM((rows, features), BF),
            pltpu.VMEM((width, features), BF),
            pltpu.VMEM((rows,), BF),
            pltpu.VMEM((width, features), F32),
            pltpu.VMEM((width, features), BF),
            pltpu.VMEM((count, pair, features), BF),
            pltpu.VMEM((2, max(count - 1, 1), pair, half), BF),
            pltpu.VMEM((2, max(count - 1, 1), pair, half), BF),
            pltpu.VMEM((chunks, chunk_rows, features), F32),
            pltpu.VMEM((2, chunks, chunk_rows, features), wire),
            pltpu.VMEM((2, chunks, chunk_rows, features), wire),
            pltpu.VMEM((chunks // 2, chunk_rows, features), F32),
            pltpu.VMEM((chunks // 2, chunk_rows, features), F32),
            pltpu.VMEM((len(stages), 1, 128), F32),
            pltpu.VMEM((2, 1, 128), F32),
            pltpu.VMEM((slots, 1, 128), F32),
            pltpu.VMEM((seq, features), F32),
            pltpu.VMEM((seq, 1), F32),
            pltpu.VMEM((rows, 1), F32),
            pltpu.VMEM((rows, 128), F32),
            dma((4,)),
            dma((7,)),
            dma((2 * count,)),
            dma((count,)),
            dma((2 * count,)),
            dma((max(count - 1, 1) * chunks,)),
            dma((4 * chunks,)),
            dma((chunks // 2,)),
            dma((1 + len(stages),)),
            pltpu.SemaphoreType.REGULAR,
        ],
        compiler_params=pltpu.CompilerParams(
            collective_id=0, has_side_effects=True, vmem_limit_bytes=40 * 1024 * 1024
        ),
    )(
        *[
            pltpu.with_memory_space_constraint(x, pltpu.HBM)
            for x in (states, cotangent, kv_weight, norm_gain)
        ],
        prompt_len, response_len, reward_bucket,
    )
    return key_values, grad_weight, grad_gain.reshape(rows)


def solution(mesh):
    placed = (
        P(("replica", "fsdp"), None, None),
        P(("replica", "fsdp"), None, None),
        P("fsdp", None),
        P("fsdp"),
        P(("replica", "fsdp")),
        P(("replica", "fsdp")),
        P(("replica", "fsdp")),
    )
    return jax.shard_map(
        functools.partial(shards, mesh.shape["replica"], mesh.shape["fsdp"]),
        mesh=mesh,
        in_specs=placed,
        out_specs=(P(("replica", "fsdp"), None, None), P("fsdp", None), P("fsdp")),
        check_vma=False,
    )
```

```python
import functools

import jax
import jax.numpy as jnp
from jax import lax
from jax.experimental import pallas as pl
from jax.experimental.pallas import tpu as pltpu
from jax.sharding import PartitionSpec as P

EPSILON = 1e-06
MESH = pl.DeviceIdType.MESH
BF = jnp.bfloat16
F32 = jnp.float32
TILE = 256
LAG = 11
HOP = 8


def flip(me, mask):
    out = me
    bit = 0
    while mask >> bit:
        if (mask >> bit) & 1:
            own = lax.rem(lax.div(me, 1 << bit), 2)
            out = out + (1 - 2 * own) * (1 << bit)
        bit += 1
    return out


def offset_of(position, order):
    count = len(order)
    return sum(((position >> (count - 1 - i)) & 1) << order[i] for i in range(count))


def plan(R, F):
    bits = F.bit_length() - 2
    count = 1 << bits
    everyone = [(k, m) for k in range(R) for m in range(count) if k or m]
    if R * count <= 32:
        stages = [everyone]
    else:
        stages = [[e for e in everyone if not e[0]], [e for e in everyone if not e[1]]]
    return bits, count, stages


def kernel(
    R, F, chunk_rows,
    states_hbm, cot_hbm, weight_hbm, gain_hbm, prompt_ref, response_ref, reward_ref,
    kv_ref, gw_ref, gg_ref,
    states, cot, scaled, weight, w_all, gain,
    grad, grad_send, grad_in, sending, receiving, own, chain_out, chain_in,
    fin_out, fin_in, scal_out, scal_pair, scal_in, acc, inverse, gcol, wide_gain,
    load_sem, send_sem, w_recv, fw_recv, g_recv, x_recv, z_recv, fin_recv, s_recv, gate,
):
    r, f = lax.axis_index("replica"), lax.axis_index("fsdp")
    bits, count, stages = plan(R, F)
    orders = (list(range(bits)), list(range(bits))[::-1])
    j = lax.div(f, 2)
    odd = lax.rem(f, 2) == 1
    seq, width = states.shape
    features = cot.shape[1]
    half = features // 2
    rows = weight.shape[0]
    pair = 2 * rows
    tiles = width // TILE
    chunks = pair // chunk_rows
    partner = (r, flip(f, 1))

    def remote(src, dst, send_sem, recv_sem, device):
        return pltpu.make_async_remote_copy(
            src_ref=src, dst_ref=dst, send_sem=send_sem, recv_sem=recv_sem,
            device_id=device, device_id_type=MESH,
        )

    def sent(ref, send_sem):
        remote(ref, ref, send_sem, send_sem, partner).wait_send()

    def got(ref, recv_sem):
        remote(ref, ref, recv_sem, recv_sem, partner).wait_recv()

    def across(bit):
        return (r, flip(f, 2 << bit))

    def peer(k, m):
        return (lax.rem(r + k, R), flip(f, m << 1))

    def pair_begin(m):
        return pl.multiple_of(flip(j, m) * pair, pair)

    loads = [
        pltpu.make_async_copy(src, dst, load_sem.at[i])
        for i, (src, dst) in enumerate([
            (gain_hbm, gain), (weight_hbm, weight), (states_hbm.at[0], states), (cot_hbm.at[0], cot),
        ])
    ]
    for copy in loads:
        copy.start()
    gain_load, weight_load, states_load, cot_load = loads

    barrier = pltpu.get_barrier_semaphore()
    pl.semaphore_signal(barrier, inc=1, device_id=partner, device_id_type=MESH)
    peers = [e for stage in stages for e in stage]

    @pl.when(odd)
    def _():
        for k, m in peers:
            pl.semaphore_signal(barrier, inc=1, device_id=peer(k, m), device_id_type=MESH)

    @pl.when(jnp.logical_not(odd))
    def _():
        for bit in range(bits):
            pl.semaphore_signal(barrier, inc=1, device_id=across(bit), device_id_type=MESH)

    lane = lax.broadcasted_iota(jnp.int32, (1, 128), 1)
    diagonal = lax.broadcasted_iota(jnp.int32, (rows, rows), 0) == lax.broadcasted_iota(
        jnp.int32, (rows, rows), 1
    )
    mine = pl.multiple_of(f * rows, rows)

    def scalars():
        reward = reward_ref[0].astype(F32)
        tokens = response_ref[0].astype(F32)
        zero = jnp.zeros((1, 128), F32)
        out = jnp.where(lane == 0, zero + reward, zero)
        out = jnp.where(lane == 1, zero + reward * reward, out)
        return jnp.where(lane == 2, zero + tokens, out), reward

    def scale_weight():
        gain_load.wait()
        row = gain[...].astype(F32).reshape(1, rows) + 1.0
        column = jnp.sum(jnp.where(diagonal, row, 0.0), axis=1, keepdims=True)
        wide_gain[...] = jnp.broadcast_to(column, wide_gain.shape)
        weight_load.wait()
        w_all[pl.ds(mine, rows), :] = (weight[...].astype(F32) * column).astype(BF)

    def scale_cotangent():
        states_load.wait()

        def square_tile(i, total):
            at = pl.multiple_of(i * TILE, TILE)
            for k in range(0, TILE, 128):
                part = states[:, pl.ds(at + k, 128)].astype(F32)
                total = total + part * part
            return total

        squares = lax.fori_loop(0, tiles, square_tile, jnp.zeros((seq, 128), F32))
        inverse[...] = lax.rsqrt(jnp.sum(squares, axis=1, keepdims=True) / width + EPSILON)
        cot_load.wait()
        position = lax.broadcasted_iota(jnp.int32, (seq, features), 0)
        first = prompt_ref[0]
        alive = (position >= first) & (position < first + response_ref[0])
        scaled[...] = jnp.where(alive, cot[...].astype(F32) * inverse[...], 0.0).astype(BF)

    def gradient(target, after):
        def tile(begin):
            at = pl.ds(pl.multiple_of(begin, TILE), TILE)
            target[at, :] = lax.dot_general(
                states[:, at], scaled[...], (((0,), (0,)), ((), ())), preferred_element_type=F32
            ).astype(target.dtype)

        def natural(i, carry):
            tile(i * TILE)
            return carry

        aligned = rows % TILE == 0
        if not aligned:
            lax.fori_loop(0, tiles, natural, 0)
        for h in range(2):
            for m in reversed(range(count)):
                begin = pair_begin(m) + h * rows
                if aligned:
                    for k in range(0, rows, TILE):
                        tile(begin + k)
                after(m, h, pl.multiple_of(begin, rows))

    def product(m, start):
        if pair % 128:
            return
        at = pl.ds(pair_begin(m), pair)
        value = jnp.dot(states[:, at], w_all[at, :], preferred_element_type=F32)
        acc[...] = value if start else acc[...] + value

    def key_values():
        if pair % 128:
            acc[...] = jnp.dot(states[...], w_all[...], preferred_element_type=F32)
        kv_ref[0] = jnp.where(inverse[...] > 0.0, acc[...] * inverse[...], 0.0).astype(BF)

    def last(order, m):
        return max(i for i in range(bits) if (m >> order[i]) & 1)

    def w_rows(m, h):
        return pl.ds(pl.multiple_of(pair_begin(m) + h * rows, rows), rows)

    def w_copy(p, m, h):
        bit = orders[p][last(orders[p], m)]
        ref = w_all.at[w_rows(m ^ (1 << bit), h), pl.ds(p * half, half)]
        return remote(ref, ref, send_sem.at[0], w_recv.at[p * count + m], across(bit))

    def hand(p, m, h):
        ref = w_all.at[w_rows(m, h), pl.ds(p * half, half)]
        remote(ref, ref, send_sem.at[1], fw_recv.at[m], partner).start()

    def handed(m, h):
        got(w_all.at[w_rows(m, h)], fw_recv.at[m])

    def received(p, m, h):
        w_copy(p, m, h).wait_recv()
        hand(p, m, h)

    def forward(p, m, h):
        for s in range(last(orders[p], m) + 1, bits):
            w_copy(p, m | (1 << orders[p][s]), h).start()

    def g_copy(m, h, begin):
        return remote(
            grad_send.at[pl.ds(begin, rows)], grad_in.at[m, pl.ds(h * rows, rows)],
            send_sem.at[2], g_recv.at[m * 2 + h], partner,
        )

    def fin_copy(c):
        return remote(fin_out.at[c], fin_in.at[c], send_sem.at[2], fin_recv.at[c], partner)

    def pair_scalars():
        return remote(scal_pair.at[0], scal_pair.at[1], send_sem.at[3], s_recv.at[0], partner)

    def finish_weight():
        sent(w_all.at[pl.ds(0, (count - 1) * rows)], send_sem.at[0])
        sent(w_all.at[pl.ds(0, count * rows)], send_sem.at[1])

    def finished(total, c):
        at = slice((c % (chunks // 2)) * chunk_rows, (c % (chunks // 2) + 1) * chunk_rows)
        column = wide_gain[at, 0:1]
        gw_ref[at, :] = total * column
        gcol[at, :] = jnp.sum(total * weight[at, :].astype(F32), axis=1, keepdims=True)

    def grad_gain():
        gg_ref[...] = jnp.sum(jnp.where(diagonal, gcol[...], 0.0), axis=0, keepdims=True)

    levels = [[m for m in range(count) if m.bit_count() == n] for n in range(bits + 1)]
    firsts = [(p, 1 << orders[p][0]) for p in range(2)]

    @pl.when(jnp.logical_not(odd))
    def _():
        pl.semaphore_wait(barrier, bits + 1)
        scal, _ = scalars()
        scal_pair[0] = scal
        pair_scalars().start()
        scale_weight()
        for s in range(bits):
            for p in range(2):
                w_copy(p, 1 << orders[p][s], 0).start()
        scale_cotangent()
        gradient(grad_send, lambda m, h, begin: g_copy(m, h, begin).start())
        for p in range(2):
            hand(p, 0, 0)
        handed(0, 1)
        product(0, True)
        for m in levels[1]:
            for p in range(2):
                received(p, m, 0)
        pl.semaphore_wait(gate, 1)
        for n in range(1, bits + 1):
            for m in levels[n]:
                for p in range(2):
                    if n > 1:
                        received(p, m, 0)
                    forward(p, m, 0)
        for n in range(1, bits + 1):
            for m in levels[n]:
                handed(m, 1)
                product(m, False)
        key_values()
        for c in range(chunks // 2):
            fin_copy(c).wait_recv()
            finished(fin_in[c], c)
        grad_gain()
        finish_weight()
        sent(grad_send, send_sem.at[2])
        sent(scal_pair.at[0], send_sem.at[3])

    @pl.when(odd)
    def _():
        pl.semaphore_wait(barrier, len(peers) + 1)
        scal, reward = scalars()
        pair_scalars().wait_recv()
        low = scal_pair[1]
        total = scal + low

        def exchange(which, total):
            first = sum(len(stage) for stage in stages[:which])
            scal_out[which] = total
            for i, (k, m) in enumerate(stages[which]):
                remote(
                    scal_out.at[which], scal_in.at[first + i], send_sem.at[3],
                    s_recv.at[1 + which], peer(k, m),
                ).start()

        def collect(which, total):
            first = sum(len(stage) for stage in stages[:which])
            size = len(stages[which])
            got(scal_in.at[pl.ds(first, size)], s_recv.at[1 + which])
            for i in range(first, first + size):
                total = total + scal_in[i]
            return total

        exchange(0, total)
        scale_weight()
        for p, m in firsts:
            w_copy(p, m, 1).start()
        for p in range(2):
            hand(p, 0, 1)
        scale_cotangent()
        gradient(grad, lambda m, h, begin: None)
        total = collect(0, total)
        for which in range(1, len(stages)):
            exchange(which, total)
            total = collect(which, total)

        def pick(source, index):
            return jnp.sum(jnp.where(lane == index, source, 0.0), axis=1, keepdims=True)

        number = float(R * F)
        average = pick(total, 0) / number
        variance = pick(total, 1) / number - average * average
        size = lax.rsqrt(variance + EPSILON) * lax.rsqrt(pick(total, 2))
        coef = (reward - average) * size
        coef_low = (pick(low, 0) - average) * size

        starts = [count - (count >> i) for i in range(bits + 1)]
        arrived = set()

        def chunk_at(c):
            return pl.ds(c * chunk_rows, chunk_rows)

        def arrive(q, c, step):
            for p in range(2):
                m, h = offset_of(q, orders[p]), c // (chunks // 2)
                if (m, h) not in arrived:
                    arrived.add((m, h))
                    g_copy(m, h, w_rows(m, h).start).wait_recv()
            for i in range(step):
                slot = starts[i] + q
                got(receiving.at[:, slot, chunk_at(c)], x_recv.at[slot * chunks + c])

        def partial(p, q, c, step):
            m = offset_of(q, orders[p])
            columns = slice(p * half, (p + 1) * half)
            begin = pl.multiple_of(pair_begin(m) + c * chunk_rows, chunk_rows)
            value = grad[pl.ds(begin, chunk_rows), columns] * coef
            value = value + grad_in[m, chunk_at(c), columns].astype(F32) * coef_low
            for i in range(step):
                value = value + receiving[p, starts[i] + q, chunk_at(c)].astype(F32)
            return value

        def scatter(step, q, c):
            keep = count >> (step + 1)
            slot = starts[step] + q
            arrive(keep + q, c, step)
            for p in range(2):
                sending[p, slot, chunk_at(c)] = partial(p, keep + q, c, step).astype(BF)
                remote(
                    sending.at[p, slot, chunk_at(c)], receiving.at[p, slot, chunk_at(c)],
                    send_sem.at[4], x_recv.at[slot * chunks + c], across(orders[p][step]),
                ).start()

        def z_copy(way, c, p):
            after = r + 1 - 2 * way
            columns = pl.ds(p * half, half)
            return remote(
                chain_out.at[way, c, :, columns], chain_in.at[way, c, :, columns],
                send_sem.at[5 + way], z_recv.at[(way * chunks + c) * 2 + p],
                (lax.rem(after + R, R), f),
            )

        def place(way):
            return r if way == 0 else R - 1 - r

        def gather_own(c):
            arrive(0, c, bits)
            for p in range(2):
                own[c, :, p * half:(p + 1) * half] = partial(p, 0, c, bits)

        def relay(hop, c):
            for way in range(2):
                @pl.when(place(way) == hop)
                def _(way=way):
                    for p in range(2):
                        columns = slice(p * half, (p + 1) * half)
                        value = own[c, :, columns]
                        if hop:
                            z_copy(way, c, p).wait_recv()
                            value = value + chain_in[way, c, :, columns].astype(F32)
                        chain_out[way, c, :, columns] = value.astype(chain_out.dtype)
                        z_copy(way, c, p).start()

        def total_of(c):
            for way in range(2):
                @pl.when(place(way) == R - 1)
                def _(way=way):
                    for p in range(2):
                        z_copy(way, c, p).wait_recv()
            value = own[c]
            for way in range(2):
                value = value + jnp.where(place(way) > 0, chain_in[way, c].astype(F32), 0.0)
            if c < chunks // 2:
                fin_out[c] = value
                fin_copy(c).start()
            else:
                finished(value, c)

        def products(n):
            for m in levels[n]:
                handed(m, 0)
                product(m, m == 0)

        def open_gate():
            pl.semaphore_signal(gate, inc=1, device_id=partner, device_id_type=MESH)

        def weight_first():
            for p, m in firsts:
                received(p, m, 1)

        def weight_second():
            for p, m in firsts:
                for s in range(1, bits):
                    w_copy(p, 1 << orders[p][s], 1).start()
                forward(p, m, 1)

        def weight_level(n):
            for m in levels[n]:
                for p in range(2):
                    if (p, m) not in firsts:
                        received(p, m, 1)
                        forward(p, m, 1)

        events = []

        def at(key, action, *arguments):
            events.append((key, len(events), action, arguments))

        period = count - 1
        final = LAG * bits
        for c in range(chunks):
            for step in range(bits):
                keep = count >> (step + 1)
                for q in reversed(range(keep)):
                    late = 6 if 2 * q < keep and step < bits - 1 else 0
                    at(period * c + LAG * step + late, scatter, step, q, c)
            at(period * c + final, gather_own, c)
            for hop in range(R - 1):
                at(period * c + final + HOP * hop, relay, hop, c)
            at(period * c + final + HOP * (R - 1), total_of, c)
        scattered = period * (chunks - 1) + LAG * (bits - 1)
        ending = period * (chunks - 1) + final + HOP * (R - 1)
        at(final, weight_first)
        at(final, products, 0)
        at(scattered, weight_second)
        at(scattered + 5, open_gate)
        for n in range(1, bits + 1):
            late = (bits - n) * HOP
            at(ending - 14 - late, weight_level, n)
            at(ending - 7 - late, products, n)
        at(ending - 7, key_values)
        for _, _, action, arguments in sorted(events, key=lambda e: e[:2]):
            action(*arguments)
        grad_gain()
        finish_weight()
        sent(fin_out, send_sem.at[2])
        sent(scal_in, send_sem.at[3])
        sent(sending, send_sem.at[4])
        for way in range(2):
            @pl.when(place(way) < R - 1)
            def _(way=way):
                sent(chain_out.at[way], send_sem.at[5 + way])


def writer(*refs):
    *pairs, sem = refs
    copies = [
        pltpu.make_async_copy(source, target, sem.at[i])
        for i, (source, target) in enumerate(zip(pairs[:3], pairs[3:]))
    ]
    for copy in copies:
        copy.start()
    for copy in copies:
        copy.wait()


def shards(R, F, states, cotangent, kv_weight, norm_gain, prompt_len, response_len, reward_bucket):
    _, seq, width = states.shape
    rows, features = kv_weight.shape
    half = features // 2
    bits, count, stages = plan(R, F)
    pair = 2 * rows
    chunk_rows = max(pair // 8, 16)
    chunks = pair // chunk_rows
    wire = BF if R <= 4 else F32
    slots = sum(len(stage) for stage in stages)
    vmem = pl.BlockSpec(memory_space=pltpu.VMEM)
    hbm = pl.BlockSpec(memory_space=pltpu.HBM)
    smem = pl.BlockSpec(memory_space=pltpu.SMEM)
    dma = pltpu.SemaphoreType.DMA
    key_values, grad_weight, grad_gain = pl.pallas_call(
        functools.partial(kernel, R, F, chunk_rows),
        out_shape=(
            jax.ShapeDtypeStruct((1, seq, features), BF),
            jax.ShapeDtypeStruct((rows, features), F32),
            jax.ShapeDtypeStruct((1, rows), F32),
        ),
        in_specs=[hbm] * 4 + [smem] * 3,
        out_specs=(vmem, vmem, vmem),
        scratch_shapes=[
            pltpu.VMEM((seq, width), BF),
            pltpu.VMEM((seq, features), BF),
            pltpu.VMEM((seq, features), BF),
            pltpu.VMEM((rows, features), BF),
            pltpu.VMEM((width, features), BF),
            pltpu.VMEM((rows,), BF),
            pltpu.VMEM((width, features), F32),
            pltpu.VMEM((width, features), BF),
            pltpu.VMEM((count, pair, features), BF),
            pltpu.VMEM((2, max(count - 1, 1), pair, half), BF),
            pltpu.VMEM((2, max(count - 1, 1), pair, half), BF),
            pltpu.VMEM((chunks, chunk_rows, features), F32),
            pltpu.VMEM((2, chunks, chunk_rows, features), wire),
            pltpu.VMEM((2, chunks, chunk_rows, features), wire),
            pltpu.VMEM((chunks // 2, chunk_rows, features), F32),
            pltpu.VMEM((chunks // 2, chunk_rows, features), F32),
            pltpu.VMEM((len(stages), 1, 128), F32),
            pltpu.VMEM((2, 1, 128), F32),
            pltpu.VMEM((slots, 1, 128), F32),
            pltpu.VMEM((seq, features), F32),
            pltpu.VMEM((seq, 1), F32),
            pltpu.VMEM((rows, 1), F32),
            pltpu.VMEM((rows, 128), F32),
            dma((4,)),
            dma((7,)),
            dma((2 * count,)),
            dma((count,)),
            dma((2 * count,)),
            dma((max(count - 1, 1) * chunks,)),
            dma((4 * chunks,)),
            dma((chunks // 2,)),
            dma((1 + len(stages),)),
            pltpu.SemaphoreType.REGULAR,
        ],
        compiler_params=pltpu.CompilerParams(
            collective_id=0, has_side_effects=True, vmem_limit_bytes=40 * 1024 * 1024
        ),
    )(
        *[
            pltpu.with_memory_space_constraint(x, pltpu.HBM)
            for x in (states, cotangent, kv_weight, norm_gain)
        ],
        prompt_len, response_len, reward_bucket,
    )
    key_values, grad_weight, grad_gain = pl.pallas_call(
        writer,
        out_shape=(
            jax.ShapeDtypeStruct(key_values.shape, BF),
            jax.ShapeDtypeStruct(grad_weight.shape, F32),
            jax.ShapeDtypeStruct(grad_gain.shape, F32),
        ),
        in_specs=[vmem] * 3,
        out_specs=(hbm,) * 3,
        scratch_shapes=[dma((3,))],
    )(*[
        pltpu.with_memory_space_constraint(x, pltpu.VMEM)
        for x in (key_values, grad_weight, grad_gain)
    ])
    return key_values, grad_weight, grad_gain.reshape(rows)


def solution(mesh):
    placed = (
        P(("replica", "fsdp"), None, None),
        P(("replica", "fsdp"), None, None),
        P("fsdp", None),
        P("fsdp"),
        P(("replica", "fsdp")),
        P(("replica", "fsdp")),
        P(("replica", "fsdp")),
    )
    return jax.shard_map(
        functools.partial(shards, mesh.shape["replica"], mesh.shape["fsdp"]),
        mesh=mesh,
        in_specs=placed,
        out_specs=(P(("replica", "fsdp"), None, None), P("fsdp", None), P("fsdp")),
        check_vma=False,
    )
```

```python
import functools

import jax
import jax.numpy as jnp
from jax import lax
from jax.experimental import pallas as pl
from jax.experimental.pallas import tpu as pltpu
from jax.sharding import PartitionSpec as P

EPSILON = 1e-06
MESH = pl.DeviceIdType.MESH
BF = jnp.bfloat16
F32 = jnp.float32
TILE = 256
LAG = 11
HOP = 8
CAST = -5
NEXT = 9
ZOFF = 1
SECOND = 0
EARLY = 2


def flip(me, mask):
    out = me
    bit = 0
    while mask >> bit:
        if (mask >> bit) & 1:
            own = lax.rem(lax.div(me, 1 << bit), 2)
            out = out + (1 - 2 * own) * (1 << bit)
        bit += 1
    return out


def offset_of(position, order):
    count = len(order)
    return sum(((position >> (count - 1 - i)) & 1) << order[i] for i in range(count))


def plan(R, F):
    bits = F.bit_length() - 2
    count = 1 << bits
    everyone = [(k, m) for k in range(R) for m in range(count) if k or m]
    if R * count <= 32:
        stages = [everyone]
    else:
        stages = [[e for e in everyone if not e[0]], [e for e in everyone if not e[1]]]
    return bits, count, stages


def kernel(
    R, F, chunk_rows, early,
    states_hbm, cot_hbm, weight_hbm, gain_hbm, prompt_ref, response_ref, reward_ref,
    kv_ref, gw_ref, gg_ref,
    states, cot, scaled, weight, w_all, gain,
    grad, grad_send, grad_in, sending, receiving, own, chain_out, chain_in,
    pre_out, pre_in, cast_out, cast_in, fin_out, fin_in, scal_out, scal_pair, scal_in, acc, inverse, gcol, wide_gain,
    load_sem, send_sem, w_recv, fw_recv, g_recv, x_recv, z_recv, pre_recv, cast_recv, fin_recv, s_recv, gate,
):
    r, f = lax.axis_index("replica"), lax.axis_index("fsdp")
    bits, count, stages = plan(R, F)
    orders = (list(range(bits)), list(range(bits))[::-1])
    j = lax.div(f, 2)
    odd = lax.rem(f, 2) == 1
    seq, width = states.shape
    features = cot.shape[1]
    half = features // 2
    rows = weight.shape[0]
    pair = 2 * rows
    tiles = width // TILE
    chunks = pair // chunk_rows
    partner = (r, flip(f, 1))

    def remote(src, dst, send_sem, recv_sem, device):
        return pltpu.make_async_remote_copy(
            src_ref=src, dst_ref=dst, send_sem=send_sem, recv_sem=recv_sem,
            device_id=device, device_id_type=MESH,
        )

    def sent(ref, send_sem):
        remote(ref, ref, send_sem, send_sem, partner).wait_send()

    def got(ref, recv_sem):
        remote(ref, ref, recv_sem, recv_sem, partner).wait_recv()

    def across(bit):
        return (r, flip(f, 2 << bit))

    def peer(k, m):
        return (lax.rem(r + k, R), flip(f, m << 1))

    def pair_begin(m):
        return pl.multiple_of(flip(j, m) * pair, pair)

    loads = [
        pltpu.make_async_copy(src, dst, load_sem.at[i])
        for i, (src, dst) in enumerate([
            (gain_hbm, gain), (weight_hbm, weight), (states_hbm.at[0], states), (cot_hbm.at[0], cot),
        ])
    ]
    for copy in loads:
        copy.start()
    gain_load, weight_load, states_load, cot_load = loads

    barrier = pltpu.get_barrier_semaphore()
    pl.semaphore_signal(barrier, inc=1, device_id=partner, device_id_type=MESH)
    peers = [e for stage in stages for e in stage]

    @pl.when(odd)
    def _():
        for k, m in peers:
            pl.semaphore_signal(barrier, inc=1, device_id=peer(k, m), device_id_type=MESH)

    @pl.when(jnp.logical_not(odd))
    def _():
        for bit in range(bits):
            pl.semaphore_signal(barrier, inc=1, device_id=across(bit), device_id_type=MESH)

    lane = lax.broadcasted_iota(jnp.int32, (1, 128), 1)
    diagonal = lax.broadcasted_iota(jnp.int32, (rows, rows), 0) == lax.broadcasted_iota(
        jnp.int32, (rows, rows), 1
    )
    mine = pl.multiple_of(f * rows, rows)

    def scalars():
        reward = reward_ref[0].astype(F32)
        tokens = response_ref[0].astype(F32)
        zero = jnp.zeros((1, 128), F32)
        out = jnp.where(lane == 0, zero + reward, zero)
        out = jnp.where(lane == 1, zero + reward * reward, out)
        return jnp.where(lane == 2, zero + tokens, out), reward

    def scale_weight():
        gain_load.wait()
        row = gain[...].astype(F32).reshape(1, rows) + 1.0
        column = jnp.sum(jnp.where(diagonal, row, 0.0), axis=1, keepdims=True)
        wide_gain[...] = jnp.broadcast_to(column, wide_gain.shape)
        weight_load.wait()
        w_all[pl.ds(mine, rows), :] = (weight[...].astype(F32) * column).astype(BF)

    def scale_cotangent():
        states_load.wait()

        def square_tile(i, total):
            at = pl.multiple_of(i * TILE, TILE)
            for k in range(0, TILE, 128):
                part = states[:, pl.ds(at + k, 128)].astype(F32)
                total = total + part * part
            return total

        squares = lax.fori_loop(0, tiles, square_tile, jnp.zeros((seq, 128), F32))
        inverse[...] = lax.rsqrt(jnp.sum(squares, axis=1, keepdims=True) / width + EPSILON)
        cot_load.wait()
        position = lax.broadcasted_iota(jnp.int32, (seq, features), 0)
        first = prompt_ref[0]
        alive = (position >= first) & (position < first + response_ref[0])
        scaled[...] = jnp.where(alive, cot[...].astype(F32) * inverse[...], 0.0).astype(BF)

    def gradient(target, after):
        def tile(begin):
            at = pl.ds(pl.multiple_of(begin, TILE), TILE)
            target[at, :] = lax.dot_general(
                states[:, at], scaled[...], (((0,), (0,)), ((), ())), preferred_element_type=F32
            ).astype(target.dtype)

        def natural(i, carry):
            tile(i * TILE)
            return carry

        aligned = rows % TILE == 0
        if not aligned:
            lax.fori_loop(0, tiles, natural, 0)
        for h in range(2):
            for m in reversed(range(count)):
                begin = pair_begin(m) + h * rows
                if aligned:
                    for k in range(0, rows, TILE):
                        tile(begin + k)
                after(m, h, pl.multiple_of(begin, rows))

    def product(m, start):
        if pair % 128:
            return
        at = pl.ds(pair_begin(m), pair)
        value = jnp.dot(states[:, at], w_all[at, :], preferred_element_type=F32)
        acc[...] = value if start else acc[...] + value

    def key_values():
        if pair % 128:
            acc[...] = jnp.dot(states[...], w_all[...], preferred_element_type=F32)
        kv_ref[0] = jnp.where(inverse[...] > 0.0, acc[...] * inverse[...], 0.0).astype(BF)

    def last(order, m):
        return max(i for i in range(bits) if (m >> order[i]) & 1)

    def w_rows(m, h):
        return pl.ds(pl.multiple_of(pair_begin(m) + h * rows, rows), rows)

    def w_copy(p, m, h):
        bit = orders[p][last(orders[p], m)]
        ref = w_all.at[w_rows(m ^ (1 << bit), h), pl.ds(p * half, half)]
        return remote(ref, ref, send_sem.at[0], w_recv.at[p * count + m], across(bit))

    def hand(p, m, h):
        ref = w_all.at[w_rows(m, h), pl.ds(p * half, half)]
        remote(ref, ref, send_sem.at[1], fw_recv.at[m], partner).start()

    def handed(m, h):
        got(w_all.at[w_rows(m, h)], fw_recv.at[m])

    def received(p, m, h):
        w_copy(p, m, h).wait_recv()
        hand(p, m, h)

    def forward(p, m, h):
        for s in range(last(orders[p], m) + 1, bits):
            w_copy(p, m | (1 << orders[p][s]), h).start()

    def g_copy(m, h, begin):
        return remote(
            grad_send.at[pl.ds(begin, rows)], grad_in.at[m, pl.ds(h * rows, rows)],
            send_sem.at[2], g_recv.at[h], partner,
        )

    def fin_copy(c):
        return remote(fin_out.at[c], fin_in.at[c], send_sem.at[2], fin_recv.at[c], partner)

    def pair_scalars():
        return remote(scal_pair.at[0], scal_pair.at[1], send_sem.at[3], s_recv.at[0], partner)

    def finish_weight():
        sent(w_all.at[pl.ds(0, (count - 1) * rows)], send_sem.at[0])
        sent(w_all.at[pl.ds(0, count * rows)], send_sem.at[1])

    def finished(total, begin):
        at = pl.ds(begin, total.shape[0])
        gw_ref[at, :] = total * wide_gain[at, 0:1]
        gcol[at, :] = jnp.sum(total * weight[at, :].astype(F32), axis=1, keepdims=True)

    def local(c):
        return (c % (chunks // 2)) * chunk_rows

    def grad_gain():
        gg_ref[...] = jnp.sum(jnp.where(diagonal, gcol[...], 0.0), axis=0, keepdims=True)

    levels = [[m for m in range(count) if m.bit_count() == n] for n in range(bits + 1)]
    firsts = [(p, 1 << orders[p][0]) for p in range(2)]

    @pl.when(jnp.logical_not(odd))
    def _():
        pl.semaphore_wait(barrier, bits + 1)
        scal, _ = scalars()
        scal_pair[0] = scal
        pair_scalars().start()
        scale_weight()
        for s in range(bits):
            for p in range(2):
                w_copy(p, 1 << orders[p][s], 0).start()
        scale_cotangent()
        gradient(grad_send, lambda m, h, begin: g_copy(m, h, begin).start())
        for p in range(2):
            hand(p, 0, 0)
        handed(0, 1)
        product(0, True)
        for m in levels[1]:
            for p in range(2):
                received(p, m, 0)
        pl.semaphore_wait(gate, 1)
        for n in range(1, bits + 1):
            for m in levels[n]:
                for p in range(2):
                    if n > 1:
                        received(p, m, 0)
                    forward(p, m, 0)
        for n in range(1, bits + 1):
            for m in levels[n]:
                handed(m, 1)
                product(m, False)
        key_values()
        for c in range(chunks // 2):
            fin_copy(c).wait_recv()
            finished(fin_in[c], local(c))
        grad_gain()
        finish_weight()
        sent(grad_send, send_sem.at[2])
        sent(scal_pair.at[0], send_sem.at[3])

    @pl.when(odd)
    def _():
        pl.semaphore_wait(barrier, len(peers) + 1)
        scal, reward = scalars()
        pair_scalars().wait_recv()
        low = scal_pair[1]
        total = scal + low

        def exchange(which, total):
            first = sum(len(stage) for stage in stages[:which])
            scal_out[which] = total
            for i, (k, m) in enumerate(stages[which]):
                remote(
                    scal_out.at[which], scal_in.at[first + i], send_sem.at[3],
                    s_recv.at[1 + which], peer(k, m),
                ).start()

        def collect(which, total):
            first = sum(len(stage) for stage in stages[:which])
            size = len(stages[which])
            got(scal_in.at[pl.ds(first, size)], s_recv.at[1 + which])
            for i in range(first, first + size):
                total = total + scal_in[i]
            return total

        exchange(0, total)
        scale_weight()
        for p, m in firsts:
            w_copy(p, m, 1).start()
        for p in range(2):
            hand(p, 0, 1)
        scale_cotangent()
        gradient(grad, lambda m, h, begin: None)
        total = collect(0, total)
        for which in range(1, len(stages)):
            exchange(which, total)
            total = collect(which, total)

        def pick(source, index):
            return jnp.sum(jnp.where(lane == index, source, 0.0), axis=1, keepdims=True)

        number = float(R * F)
        average = pick(total, 0) / number
        variance = pick(total, 1) / number - average * average
        size = lax.rsqrt(variance + EPSILON) * lax.rsqrt(pick(total, 2))
        coef = (reward - average) * size
        coef_low = (pick(low, 0) - average) * size

        starts = [count - (count >> i) for i in range(bits + 1)]
        arrived, halves = set(), set()

        part = chunk_rows // 2
        rounds = R.bit_length() - 1
        side = lax.rem(r, 2)

        def height(c):
            return part if c < early else chunk_rows

        def chunk_at(c):
            return pl.ds(c * chunk_rows, height(c))

        def need(m, h):
            if h not in halves:
                halves.add(h)
                got(grad_in.at[:, pl.ds(h * rows, rows)], g_recv.at[h])

        def scaled_rows(m, begin, size, columns):
            at = pl.ds(pl.multiple_of(pair_begin(m) + begin, size), size)
            value = grad[at, columns] * coef
            at = pl.ds(pl.multiple_of(begin, size), size)
            return value + grad_in[m, at, columns].astype(F32) * coef_low

        def pre_copy(c):
            return remote(
                pre_out.at[c], pre_in.at[c], send_sem.at[7], pre_recv.at[c],
                (r + 1 - 2 * side, f),
            )

        def pre_sum(c):
            for m in range(count):
                need(m, c // (chunks // 2))
                begin = c * chunk_rows + (1 - side) * part
                pre_out[c, m] = scaled_rows(m, begin, part, slice(0, features)).astype(BF)
            pre_copy(c).start()

        def arrive(q, c, step):
            for p in range(2):
                need(offset_of(q, orders[p]), c // (chunks // 2))
            if c < early and c not in arrived:
                arrived.add(c)
                pre_copy(c).wait_recv()
            if step:
                got(receiving.at[:, pl.ds(0, step), chunk_at(c)], x_recv.at[q * chunks + c])

        def partial(p, q, c, step):
            m = offset_of(q, orders[p])
            columns = slice(p * half, (p + 1) * half)
            if c < early:
                value = scaled_rows(m, c * chunk_rows + side * part, part, columns)
                value = value + pre_in[c, m, :, columns].astype(F32)
            else:
                value = scaled_rows(m, c * chunk_rows, chunk_rows, columns)
            for i in range(step):
                value = value + receiving[p, starts[i] + q, chunk_at(c)].astype(F32)
            return value

        def scatter(step, q, c):
            keep = count >> (step + 1)
            slot = starts[step] + q
            arrive(keep + q, c, step)
            for p in range(2):
                sending[p, slot, chunk_at(c)] = partial(p, keep + q, c, step).astype(BF)
                remote(
                    sending.at[p, slot, chunk_at(c)], receiving.at[p, slot, chunk_at(c)],
                    send_sem.at[8 if c < early else 4], x_recv.at[q * chunks + c],
                    across(orders[p][step]),
                ).start()

        def cast_copy(step, c):
            k = 1 << step if step else 0
            device = (lax.rem(r + k, R), f) if step else (r + 1 - 2 * side, f)
            return remote(
                cast_out.at[c, step], cast_in.at[c, step], send_sem.at[9],
                cast_recv.at[c * rounds + step], device,
            )

        def cast(step, c):
            if step == rounds - 1:
                arrive(0, c, bits)
                for p in range(2):
                    own[c, 0:part, p * half:(p + 1) * half] = partial(p, 0, c, bits)
            else:
                cast_copy(step + 1, c).wait_recv()
                own[c, 0:part] = own[c, 0:part] + cast_in[c, step + 1].astype(F32)
            cast_out[c, step] = own[c, 0:part].astype(BF)
            cast_copy(step, c).start()

        def cast_total(c):
            cast_copy(0, c).wait_recv()
            for value, at in ((own[c, 0:part], side), (cast_in[c, 0].astype(F32), 1 - side)):
                begin = pl.multiple_of(at * part, part)
                if c < chunks // 2:
                    fin_out[c, pl.ds(begin, part), :] = value
                else:
                    finished(value, pl.multiple_of(local(c) + begin, part))
            if c < chunks // 2:
                fin_copy(c).start()

        def z_copy(way, c, p):
            after = r + 1 - 2 * way
            columns = pl.ds(p * half, half)
            return remote(
                chain_out.at[way, c, :, columns], chain_in.at[way, c, :, columns],
                send_sem.at[5 + way], z_recv.at[(way * (chunks - early) + c - early) * 2 + p],
                (lax.rem(after + R, R), f),
            )

        def place(way):
            return r if way == 0 else R - 1 - r

        def gather_own(c):
            arrive(0, c, bits)
            for p in range(2):
                own[c, :, p * half:(p + 1) * half] = partial(p, 0, c, bits)

        def relay(hop, c):
            for way in range(2):
                @pl.when(place(way) == hop)
                def _(way=way):
                    for p in range(2):
                        columns = slice(p * half, (p + 1) * half)
                        value = own[c, :, columns]
                        if hop:
                            z_copy(way, c, p).wait_recv()
                            value = value + chain_in[way, c, :, columns].astype(F32)
                        chain_out[way, c, :, columns] = value.astype(chain_out.dtype)
                        z_copy(way, c, p).start()

        def total_of(c):
            for way in range(2):
                @pl.when(place(way) == R - 1)
                def _(way=way):
                    for p in range(2):
                        z_copy(way, c, p).wait_recv()
            value = own[c]
            for way in range(2):
                value = value + jnp.where(place(way) > 0, chain_in[way, c].astype(F32), 0.0)
            if c < chunks // 2:
                fin_out[c] = value
                fin_copy(c).start()
            else:
                finished(value, local(c))

        def products(n):
            for m in levels[n]:
                handed(m, 0)
                product(m, m == 0)

        def open_gate():
            pl.semaphore_signal(gate, inc=1, device_id=partner, device_id_type=MESH)

        def weight_first():
            for p, m in firsts:
                received(p, m, 1)

        def weight_second():
            for p, m in firsts:
                for s in range(1, bits):
                    w_copy(p, 1 << orders[p][s], 1).start()
                forward(p, m, 1)

        def weight_level(n):
            for m in levels[n]:
                for p in range(2):
                    if (p, m) not in firsts:
                        received(p, m, 1)
                        forward(p, m, 1)

        events = []

        def at(key, action, *arguments):
            events.append((key, len(events), action, arguments))

        period = count - 1
        final = LAG * bits
        scattered = ending = 0
        for c in range(chunks):
            base = period * (c - early)
            if c < early:
                base = period * (chunks - early + c) + ZOFF
                at(4 * c, pre_sum, c)
            for step in range(bits):
                keep = count >> (step + 1)
                for q in reversed(range(keep)):
                    late = 6 if 2 * q < keep and step < bits - 1 else 0
                    at(base + LAG * step + late, scatter, step, q, c)
                    scattered = max(scattered, base + LAG * step + late)
            if c < early:
                for step in reversed(range(rounds)):
                    at(base + final + CAST + (rounds - 1 - step) * NEXT, cast, step, c)
                at(base + final + CAST + rounds * HOP, cast_total, c)
                continue
            at(base + final, gather_own, c)
            for hop in range(R - 1):
                at(base + final + HOP * hop, relay, hop, c)
            at(base + final + HOP * (R - 1), total_of, c)
            ending = max(ending, base + final + HOP * (R - 1))
        at(final, weight_first)
        at(final, products, 0)
        at(scattered + SECOND, weight_second)
        at(scattered + 2, open_gate)
        for n in range(1, bits + 1):
            at(ending - 7 - 6 * (bits - n), weight_level, n)
            at(ending - 2 - 4 * (bits - n), products, n)
        at(ending - 2, key_values)
        for _, _, action, arguments in sorted(events, key=lambda e: e[:2]):
            action(*arguments)
        grad_gain()
        finish_weight()
        sent(fin_out, send_sem.at[2])
        sent(scal_in, send_sem.at[3])
        sent(sending.at[:, :, pl.ds(0, (chunks - early) * chunk_rows)], send_sem.at[4])
        if early:
            sent(pre_out, send_sem.at[7])
            sent(sending.at[:, :, pl.ds(0, early * part)], send_sem.at[8])
            sent(cast_in, send_sem.at[9])
        for way in range(2):
            @pl.when(place(way) < R - 1)
            def _(way=way):
                sent(chain_out.at[way, pl.ds(0, chunks - early)], send_sem.at[5 + way])


def writer(*refs):
    *pairs, sem = refs
    copies = [
        pltpu.make_async_copy(source, target, sem.at[i])
        for i, (source, target) in enumerate(zip(pairs[:3], pairs[3:]))
    ]
    for copy in copies:
        copy.start()
    for copy in copies:
        copy.wait()


def shards(R, F, states, cotangent, kv_weight, norm_gain, prompt_len, response_len, reward_bucket):
    _, seq, width = states.shape
    rows, features = kv_weight.shape
    half = features // 2
    bits, count, stages = plan(R, F)
    pair = 2 * rows
    chunk_rows = max(pair // 8, 16)
    chunks = pair // chunk_rows
    wire = BF if R <= 4 else F32
    early = EARLY if R in (2, 4) else 0
    some = max(early, 1)
    part = chunk_rows // 2
    rounds = max(R.bit_length() - 1, 1)
    slots = sum(len(stage) for stage in stages)
    vmem = pl.BlockSpec(memory_space=pltpu.VMEM)
    hbm = pl.BlockSpec(memory_space=pltpu.HBM)
    smem = pl.BlockSpec(memory_space=pltpu.SMEM)
    dma = pltpu.SemaphoreType.DMA
    key_values, grad_weight, grad_gain = pl.pallas_call(
        functools.partial(kernel, R, F, chunk_rows, early),
        out_shape=(
            jax.ShapeDtypeStruct((1, seq, features), BF),
            jax.ShapeDtypeStruct((rows, features), F32),
            jax.ShapeDtypeStruct((1, rows), F32),
        ),
        in_specs=[hbm] * 4 + [smem] * 3,
        out_specs=(vmem, vmem, vmem),
        scratch_shapes=[
            pltpu.VMEM((seq, width), BF),
            pltpu.VMEM((seq, features), BF),
            pltpu.VMEM((seq, features), BF),
            pltpu.VMEM((rows, features), BF),
            pltpu.VMEM((width, features), BF),
            pltpu.VMEM((rows,), BF),
            pltpu.VMEM((width, features), F32),
            pltpu.VMEM((width, features), BF),
            pltpu.VMEM((count, pair, features), BF),
            pltpu.VMEM((2, max(count - 1, 1), pair, half), BF),
            pltpu.VMEM((2, max(count - 1, 1), pair, half), BF),
            pltpu.VMEM((chunks, chunk_rows, features), F32),
            pltpu.VMEM((2, chunks, chunk_rows, features), wire),
            pltpu.VMEM((2, chunks, chunk_rows, features), wire),
            pltpu.VMEM((some, count, part, features), BF),
            pltpu.VMEM((some, count, part, features), BF),
            pltpu.VMEM((some, rounds, part, features), BF),
            pltpu.VMEM((some, rounds, part, features), BF),
            pltpu.VMEM((chunks // 2, chunk_rows, features), F32),
            pltpu.VMEM((chunks // 2, chunk_rows, features), F32),
            pltpu.VMEM((len(stages), 1, 128), F32),
            pltpu.VMEM((2, 1, 128), F32),
            pltpu.VMEM((slots, 1, 128), F32),
            pltpu.VMEM((seq, features), F32),
            pltpu.VMEM((seq, 1), F32),
            pltpu.VMEM((rows, 1), F32),
            pltpu.VMEM((rows, 128), F32),
            dma((4,)),
            dma((10,)),
            dma((2 * count,)),
            dma((count,)),
            dma((2,)),
            dma((max(count // 2, 1) * chunks,)),
            dma((4 * (chunks - early),)),
            dma((some,)),
            dma((some * rounds,)),
            dma((chunks // 2,)),
            dma((1 + len(stages),)),
            pltpu.SemaphoreType.REGULAR,
        ],
        compiler_params=pltpu.CompilerParams(
            collective_id=0, has_side_effects=True, vmem_limit_bytes=40 * 1024 * 1024
        ),
    )(
        *[
            pltpu.with_memory_space_constraint(x, pltpu.HBM)
            for x in (states, cotangent, kv_weight, norm_gain)
        ],
        prompt_len, response_len, reward_bucket,
    )
    key_values, grad_weight, grad_gain = pl.pallas_call(
        writer,
        out_shape=(
            jax.ShapeDtypeStruct(key_values.shape, BF),
            jax.ShapeDtypeStruct(grad_weight.shape, F32),
            jax.ShapeDtypeStruct(grad_gain.shape, F32),
        ),
        in_specs=[vmem] * 3,
        out_specs=(hbm,) * 3,
        scratch_shapes=[dma((3,))],
    )(*[
        pltpu.with_memory_space_constraint(x, pltpu.VMEM)
        for x in (key_values, grad_weight, grad_gain)
    ])
    return key_values, grad_weight, grad_gain.reshape(rows)


def solution(mesh):
    placed = (
        P(("replica", "fsdp"), None, None),
        P(("replica", "fsdp"), None, None),
        P("fsdp", None),
        P("fsdp"),
        P(("replica", "fsdp")),
        P(("replica", "fsdp")),
        P(("replica", "fsdp")),
    )
    return jax.shard_map(
        functools.partial(shards, mesh.shape["replica"], mesh.shape["fsdp"]),
        mesh=mesh,
        in_specs=placed,
        out_specs=(P(("replica", "fsdp"), None, None), P("fsdp", None), P("fsdp")),
        check_vma=False,
    )
```

```python
import functools

import jax
import jax.numpy as jnp
from jax import lax
from jax.experimental import pallas as pl
from jax.experimental.pallas import tpu as pltpu
from jax.sharding import PartitionSpec as P

EPSILON = 1e-06
MESH = pl.DeviceIdType.MESH
BF = jnp.bfloat16
F32 = jnp.float32
TILE = 256
LAG = 11
HOP = 8
CAST = -5
FIRST = -3.5
NEXT = 9
ZOFF = 1
SECOND = 0
EARLY = 2


def flip(me, mask):
    out = me
    bit = 0
    while mask >> bit:
        if (mask >> bit) & 1:
            own = lax.rem(lax.div(me, 1 << bit), 2)
            out = out + (1 - 2 * own) * (1 << bit)
        bit += 1
    return out


def offset_of(position, order):
    count = len(order)
    return sum(((position >> (count - 1 - i)) & 1) << order[i] for i in range(count))


def plan(R, F):
    bits = F.bit_length() - 2
    count = 1 << bits
    everyone = [(k, m) for k in range(R) for m in range(count) if k or m]
    if R * count <= 32:
        stages = [everyone]
    else:
        stages = [[e for e in everyone if not e[0]], [e for e in everyone if not e[1]]]
    return bits, count, stages


def kernel(
    R, F, chunk_rows, early,
    states_hbm, cot_hbm, weight_hbm, gain_hbm, prompt_ref, response_ref, reward_ref,
    kv_ref, gw_ref, gg_ref,
    states, cot, scaled, weight, w_all, gain,
    grad, grad_send, grad_in, sending, receiving, own, chain_out, chain_in,
    pre_out, pre_in, cast_out, cast_in, fin_out, fin_in, scal_out, scal_pair, scal_in, acc, inverse, gcol, wide_gain,
    load_sem, send_sem, w_recv, fw_recv, g_recv, x_recv, z_recv, pre_recv, cast_recv, fin_recv, s_recv, gate,
):
    r, f = lax.axis_index("replica"), lax.axis_index("fsdp")
    bits, count, stages = plan(R, F)
    orders = (list(range(bits)), list(range(bits))[::-1])
    j = lax.div(f, 2)
    odd = lax.rem(f, 2) == 1
    seq, width = states.shape
    features = cot.shape[1]
    half = features // 2
    rows = weight.shape[0]
    pair = 2 * rows
    tiles = width // TILE
    chunks = pair // chunk_rows
    partner = (r, flip(f, 1))

    def remote(src, dst, send_sem, recv_sem, device):
        return pltpu.make_async_remote_copy(
            src_ref=src, dst_ref=dst, send_sem=send_sem, recv_sem=recv_sem,
            device_id=device, device_id_type=MESH,
        )

    def sent(ref, send_sem):
        remote(ref, ref, send_sem, send_sem, partner).wait_send()

    def got(ref, recv_sem):
        remote(ref, ref, recv_sem, recv_sem, partner).wait_recv()

    def across(bit):
        return (r, flip(f, 2 << bit))

    def peer(k, m):
        return (lax.rem(r + k, R), flip(f, m << 1))

    def pair_begin(m):
        return pl.multiple_of(flip(j, m) * pair, pair)

    loads = [
        pltpu.make_async_copy(src, dst, load_sem.at[i])
        for i, (src, dst) in enumerate([
            (gain_hbm, gain), (weight_hbm, weight), (states_hbm.at[0], states), (cot_hbm.at[0], cot),
        ])
    ]
    for copy in loads:
        copy.start()
    gain_load, weight_load, states_load, cot_load = loads

    barrier = pltpu.get_barrier_semaphore()
    pl.semaphore_signal(barrier, inc=1, device_id=partner, device_id_type=MESH)
    peers = [e for stage in stages for e in stage]

    @pl.when(odd)
    def _():
        for k, m in peers:
            pl.semaphore_signal(barrier, inc=1, device_id=peer(k, m), device_id_type=MESH)

    @pl.when(jnp.logical_not(odd))
    def _():
        for bit in range(bits):
            pl.semaphore_signal(barrier, inc=1, device_id=across(bit), device_id_type=MESH)

    lane = lax.broadcasted_iota(jnp.int32, (1, 128), 1)
    diagonal = lax.broadcasted_iota(jnp.int32, (rows, rows), 0) == lax.broadcasted_iota(
        jnp.int32, (rows, rows), 1
    )
    mine = pl.multiple_of(f * rows, rows)

    def scalars():
        reward = reward_ref[0].astype(F32)
        tokens = response_ref[0].astype(F32)
        zero = jnp.zeros((1, 128), F32)
        out = jnp.where(lane == 0, zero + reward, zero)
        out = jnp.where(lane == 1, zero + reward * reward, out)
        return jnp.where(lane == 2, zero + tokens, out), reward

    def scale_weight():
        gain_load.wait()
        row = gain[...].astype(F32).reshape(1, rows) + 1.0
        column = jnp.sum(jnp.where(diagonal, row, 0.0), axis=1, keepdims=True)
        wide_gain[...] = jnp.broadcast_to(column, wide_gain.shape)
        weight_load.wait()
        w_all[pl.ds(mine, rows), :] = (weight[...].astype(F32) * column).astype(BF)

    def scale_cotangent():
        states_load.wait()

        def square_tile(i, total):
            at = pl.multiple_of(i * TILE, TILE)
            for k in range(0, TILE, 128):
                part = states[:, pl.ds(at + k, 128)].astype(F32)
                total = total + part * part
            return total

        squares = lax.fori_loop(0, tiles, square_tile, jnp.zeros((seq, 128), F32))
        inverse[...] = lax.rsqrt(jnp.sum(squares, axis=1, keepdims=True) / width + EPSILON)
        cot_load.wait()
        position = lax.broadcasted_iota(jnp.int32, (seq, features), 0)
        first = prompt_ref[0]
        alive = (position >= first) & (position < first + response_ref[0])
        scaled[...] = jnp.where(alive, cot[...].astype(F32) * inverse[...], 0.0).astype(BF)

    def gradient(target, after):
        def tile(begin):
            at = pl.ds(pl.multiple_of(begin, TILE), TILE)
            target[at, :] = lax.dot_general(
                states[:, at], scaled[...], (((0,), (0,)), ((), ())), preferred_element_type=F32
            ).astype(target.dtype)

        def natural(i, carry):
            tile(i * TILE)
            return carry

        aligned = rows % TILE == 0
        if not aligned:
            lax.fori_loop(0, tiles, natural, 0)
        for h in range(2):
            for m in reversed(range(count)):
                begin = pair_begin(m) + h * rows
                if aligned:
                    for k in range(0, rows, TILE):
                        tile(begin + k)
                after(m, h, pl.multiple_of(begin, rows))

    def product(m, start):
        if pair % 128:
            return
        at = pl.ds(pair_begin(m), pair)
        value = jnp.dot(states[:, at], w_all[at, :], preferred_element_type=F32)
        acc[...] = value if start else acc[...] + value

    def key_values():
        if pair % 128:
            acc[...] = jnp.dot(states[...], w_all[...], preferred_element_type=F32)
        kv_ref[0] = jnp.where(inverse[...] > 0.0, acc[...] * inverse[...], 0.0).astype(BF)

    def last(order, m):
        return max(i for i in range(bits) if (m >> order[i]) & 1)

    def w_rows(m, h):
        return pl.ds(pl.multiple_of(pair_begin(m) + h * rows, rows), rows)

    def w_copy(p, m, h):
        bit = orders[p][last(orders[p], m)]
        ref = w_all.at[w_rows(m ^ (1 << bit), h), pl.ds(p * half, half)]
        return remote(ref, ref, send_sem.at[0], w_recv.at[p * count + m], across(bit))

    def hand(p, m, h):
        ref = w_all.at[w_rows(m, h), pl.ds(p * half, half)]
        remote(ref, ref, send_sem.at[1], fw_recv.at[m], partner).start()

    def handed(m, h):
        got(w_all.at[w_rows(m, h)], fw_recv.at[m])

    def received(p, m, h):
        w_copy(p, m, h).wait_recv()
        hand(p, m, h)

    def forward(p, m, h):
        for s in range(last(orders[p], m) + 1, bits):
            w_copy(p, m | (1 << orders[p][s]), h).start()

    def g_copy(m, h, begin):
        return remote(
            grad_send.at[pl.ds(begin, rows)], grad_in.at[m, pl.ds(h * rows, rows)],
            send_sem.at[2], g_recv.at[h], partner,
        )

    def fin_copy(c):
        return remote(fin_out.at[c], fin_in.at[c], send_sem.at[2], fin_recv.at[c], partner)

    def pair_scalars():
        return remote(scal_pair.at[0], scal_pair.at[1], send_sem.at[3], s_recv.at[0], partner)

    def finish_weight():
        sent(w_all.at[pl.ds(0, (count - 1) * rows)], send_sem.at[0])
        sent(w_all.at[pl.ds(0, count * rows)], send_sem.at[1])

    def finished(total, begin):
        at = pl.ds(begin, total.shape[0])
        gw_ref[at, :] = total * wide_gain[at, 0:1]
        gcol[at, :] = jnp.sum(total * weight[at, :].astype(F32), axis=1, keepdims=True)

    def local(c):
        return (c % (chunks // 2)) * chunk_rows

    def grad_gain():
        gg_ref[...] = jnp.sum(jnp.where(diagonal, gcol[...], 0.0), axis=0, keepdims=True)

    levels = [[m for m in range(count) if m.bit_count() == n] for n in range(bits + 1)]
    firsts = [(p, 1 << orders[p][0]) for p in range(2)]

    @pl.when(jnp.logical_not(odd))
    def _():
        pl.semaphore_wait(barrier, bits + 1)
        scal, _ = scalars()
        scal_pair[0] = scal
        pair_scalars().start()
        scale_weight()
        for s in range(bits):
            for p in range(2):
                w_copy(p, 1 << orders[p][s], 0).start()
        scale_cotangent()
        gradient(grad_send, lambda m, h, begin: g_copy(m, h, begin).start())
        for p in range(2):
            hand(p, 0, 0)
        handed(0, 1)
        product(0, True)
        for m in levels[1]:
            for p in range(2):
                received(p, m, 0)
        pl.semaphore_wait(gate, 1)
        for n in range(1, bits + 1):
            for m in levels[n]:
                for p in range(2):
                    if n > 1:
                        received(p, m, 0)
                    forward(p, m, 0)
        for n in range(1, bits + 1):
            for m in levels[n]:
                handed(m, 1)
                product(m, False)
        key_values()
        for c in range(chunks // 2):
            fin_copy(c).wait_recv()
            finished(fin_in[c], local(c))
        grad_gain()
        finish_weight()
        sent(grad_send, send_sem.at[2])
        sent(scal_pair.at[0], send_sem.at[3])

    @pl.when(odd)
    def _():
        pl.semaphore_wait(barrier, len(peers) + 1)
        scal, reward = scalars()
        pair_scalars().wait_recv()
        low = scal_pair[1]
        total = scal + low

        def exchange(which, total):
            first = sum(len(stage) for stage in stages[:which])
            scal_out[which] = total
            for i, (k, m) in enumerate(stages[which]):
                remote(
                    scal_out.at[which], scal_in.at[first + i], send_sem.at[3],
                    s_recv.at[1 + which], peer(k, m),
                ).start()

        def collect(which, total):
            first = sum(len(stage) for stage in stages[:which])
            size = len(stages[which])
            got(scal_in.at[pl.ds(first, size)], s_recv.at[1 + which])
            for i in range(first, first + size):
                total = total + scal_in[i]
            return total

        exchange(0, total)
        scale_weight()
        for p, m in firsts:
            w_copy(p, m, 1).start()
        for p in range(2):
            hand(p, 0, 1)
        scale_cotangent()
        gradient(grad, lambda m, h, begin: None)
        total = collect(0, total)
        for which in range(1, len(stages)):
            exchange(which, total)
            total = collect(which, total)

        def pick(source, index):
            return jnp.sum(jnp.where(lane == index, source, 0.0), axis=1, keepdims=True)

        number = float(R * F)
        average = pick(total, 0) / number
        variance = pick(total, 1) / number - average * average
        size = lax.rsqrt(variance + EPSILON) * lax.rsqrt(pick(total, 2))
        coef = (reward - average) * size
        coef_low = (pick(low, 0) - average) * size

        starts = [count - (count >> i) for i in range(bits + 1)]
        arrived, halves = set(), set()

        part = chunk_rows // 2
        rounds = R.bit_length() - 1
        side = lax.rem(r, 2)

        def height(c):
            return part if c < early else chunk_rows

        def chunk_at(c):
            return pl.ds(c * chunk_rows, height(c))

        def need(m, h):
            if h not in halves:
                halves.add(h)
                got(grad_in.at[:, pl.ds(h * rows, rows)], g_recv.at[h])

        def scaled_rows(m, begin, size, columns):
            at = pl.ds(pl.multiple_of(pair_begin(m) + begin, size), size)
            value = grad[at, columns] * coef
            at = pl.ds(pl.multiple_of(begin, size), size)
            return value + grad_in[m, at, columns].astype(F32) * coef_low

        def pre_copy(c):
            return remote(
                pre_out.at[c], pre_in.at[c], send_sem.at[7], pre_recv.at[c],
                (r + 1 - 2 * side, f),
            )

        def pre_sum(c):
            for m in range(count):
                need(m, c // (chunks // 2))
                begin = c * chunk_rows + (1 - side) * part
                pre_out[c, m] = scaled_rows(m, begin, part, slice(0, features)).astype(BF)
            pre_copy(c).start()

        def arrive(q, c, step):
            for p in range(2):
                need(offset_of(q, orders[p]), c // (chunks // 2))
            if c < early and c not in arrived:
                arrived.add(c)
                pre_copy(c).wait_recv()
            if step:
                got(receiving.at[:, pl.ds(0, step), chunk_at(c)], x_recv.at[q * chunks + c])

        def partial(p, q, c, step):
            m = offset_of(q, orders[p])
            columns = slice(p * half, (p + 1) * half)
            if c < early:
                value = scaled_rows(m, c * chunk_rows + side * part, part, columns)
                value = value + pre_in[c, m, :, columns].astype(F32)
            else:
                value = scaled_rows(m, c * chunk_rows, chunk_rows, columns)
            for i in range(step):
                value = value + receiving[p, starts[i] + q, chunk_at(c)].astype(F32)
            return value

        def scatter(step, q, c):
            keep = count >> (step + 1)
            slot = starts[step] + q
            arrive(keep + q, c, step)
            for p in range(2):
                sending[p, slot, chunk_at(c)] = partial(p, keep + q, c, step).astype(BF)
                remote(
                    sending.at[p, slot, chunk_at(c)], receiving.at[p, slot, chunk_at(c)],
                    send_sem.at[8 if c < early else 4], x_recv.at[q * chunks + c],
                    across(orders[p][step]),
                ).start()

        def cast_copy(step, c):
            k = 1 << step if step else 0
            device = (lax.rem(r + k, R), f) if step else (r + 1 - 2 * side, f)
            return remote(
                cast_out.at[c, step], cast_in.at[c, step], send_sem.at[9],
                cast_recv.at[c * rounds + step], device,
            )

        def cast(step, c):
            if step == rounds - 1:
                arrive(0, c, bits)
                for p in range(2):
                    own[c, 0:part, p * half:(p + 1) * half] = partial(p, 0, c, bits)
            else:
                cast_copy(step + 1, c).wait_recv()
                own[c, 0:part] = own[c, 0:part] + cast_in[c, step + 1].astype(F32)
            cast_out[c, step] = own[c, 0:part].astype(BF)
            cast_copy(step, c).start()

        def cast_total(c):
            cast_copy(0, c).wait_recv()
            for value, at in ((own[c, 0:part], side), (cast_in[c, 0].astype(F32), 1 - side)):
                begin = pl.multiple_of(at * part, part)
                if c < chunks // 2:
                    fin_out[c, pl.ds(begin, part), :] = value
                else:
                    finished(value, pl.multiple_of(local(c) + begin, part))
            if c < chunks // 2:
                fin_copy(c).start()

        def z_copy(way, c, p):
            after = r + 1 - 2 * way
            columns = pl.ds(p * half, half)
            return remote(
                chain_out.at[way, c, :, columns], chain_in.at[way, c, :, columns],
                send_sem.at[5 + way], z_recv.at[(way * (chunks - early) + c - early) * 2 + p],
                (lax.rem(after + R, R), f),
            )

        def place(way):
            return r if way == 0 else R - 1 - r

        def gather_own(c):
            arrive(0, c, bits)
            for p in range(2):
                own[c, :, p * half:(p + 1) * half] = partial(p, 0, c, bits)

        def relay(hop, c):
            for way in range(2):
                @pl.when(place(way) == hop)
                def _(way=way):
                    for p in range(2):
                        columns = slice(p * half, (p + 1) * half)
                        value = own[c, :, columns]
                        if hop:
                            z_copy(way, c, p).wait_recv()
                            value = value + chain_in[way, c, :, columns].astype(F32)
                        chain_out[way, c, :, columns] = value.astype(chain_out.dtype)
                        z_copy(way, c, p).start()

        def total_of(c):
            for way in range(2):
                @pl.when(place(way) == R - 1)
                def _(way=way):
                    for p in range(2):
                        z_copy(way, c, p).wait_recv()
            value = own[c]
            for way in range(2):
                value = value + jnp.where(place(way) > 0, chain_in[way, c].astype(F32), 0.0)
            if c < chunks // 2:
                fin_out[c] = value
                fin_copy(c).start()
            else:
                finished(value, local(c))

        def products(n):
            for m in levels[n]:
                handed(m, 0)
                product(m, m == 0)

        def open_gate():
            pl.semaphore_signal(gate, inc=1, device_id=partner, device_id_type=MESH)

        def weight_first():
            for p, m in firsts:
                received(p, m, 1)

        def weight_second():
            for p, m in firsts:
                for s in range(1, bits):
                    w_copy(p, 1 << orders[p][s], 1).start()
                forward(p, m, 1)

        def weight_level(n):
            for m in levels[n]:
                for p in range(2):
                    if (p, m) not in firsts:
                        received(p, m, 1)
                        forward(p, m, 1)

        events = []

        def at(key, action, *arguments):
            events.append((key, len(events), action, arguments))

        period = count - 1
        final = LAG * bits
        scattered = ending = 0
        for c in range(chunks):
            base = period * (c - early)
            if c < early:
                base = period * (chunks - early + c) + ZOFF
                at(6 * c + 4, pre_sum, c)
            for step in range(bits):
                keep = count >> (step + 1)
                for q in reversed(range(keep)):
                    late = 6 if 2 * q < keep and step < bits - 1 else 0
                    at(base + LAG * step + late, scatter, step, q, c)
                    scattered = max(scattered, base + LAG * step + late)
            if c < early:
                for step in reversed(range(rounds)):
                    at(base + final + (FIRST if step == rounds - 1 else CAST + (rounds - 1 - step) * NEXT), cast, step, c)
                at(base + final + CAST + rounds * HOP, cast_total, c)
                continue
            at(base + final, gather_own, c)
            for hop in range(R - 1):
                at(base + final + HOP * hop, relay, hop, c)
            at(base + final + HOP * (R - 1), total_of, c)
            ending = max(ending, base + final + HOP * (R - 1))
        at(final, weight_first)
        at(final, products, 0)
        at(scattered + SECOND, weight_second)
        at(scattered + 2, open_gate)
        for n in range(1, bits + 1):
            at(ending - 7 - 6 * (bits - n), weight_level, n)
            at(ending - 2 - 4 * (bits - n), products, n)
        at(ending - 2, key_values)
        for _, _, action, arguments in sorted(events, key=lambda e: e[:2]):
            action(*arguments)
        grad_gain()
        finish_weight()
        sent(fin_out, send_sem.at[2])
        sent(scal_in, send_sem.at[3])
        sent(sending.at[:, :, pl.ds(0, (chunks - early) * chunk_rows)], send_sem.at[4])
        if early:
            sent(pre_out, send_sem.at[7])
            sent(sending.at[:, :, pl.ds(0, early * part)], send_sem.at[8])
            sent(cast_in, send_sem.at[9])
        for way in range(2):
            @pl.when(place(way) < R - 1)
            def _(way=way):
                sent(chain_out.at[way, pl.ds(0, chunks - early)], send_sem.at[5 + way])


def writer(*refs):
    *pairs, sem = refs
    copies = [
        pltpu.make_async_copy(source, target, sem.at[i])
        for i, (source, target) in enumerate(zip(pairs[:3], pairs[3:]))
    ]
    for copy in copies:
        copy.start()
    for copy in copies:
        copy.wait()


def shards(R, F, states, cotangent, kv_weight, norm_gain, prompt_len, response_len, reward_bucket):
    _, seq, width = states.shape
    rows, features = kv_weight.shape
    half = features // 2
    bits, count, stages = plan(R, F)
    pair = 2 * rows
    chunk_rows = max(pair // 8, 16)
    chunks = pair // chunk_rows
    wire = BF if R <= 4 else F32
    early = EARLY if R in (2, 4) else 0
    some = max(early, 1)
    part = chunk_rows // 2
    rounds = max(R.bit_length() - 1, 1)
    slots = sum(len(stage) for stage in stages)
    vmem = pl.BlockSpec(memory_space=pltpu.VMEM)
    hbm = pl.BlockSpec(memory_space=pltpu.HBM)
    smem = pl.BlockSpec(memory_space=pltpu.SMEM)
    dma = pltpu.SemaphoreType.DMA
    key_values, grad_weight, grad_gain = pl.pallas_call(
        functools.partial(kernel, R, F, chunk_rows, early),
        out_shape=(
            jax.ShapeDtypeStruct((1, seq, features), BF),
            jax.ShapeDtypeStruct((rows, features), F32),
            jax.ShapeDtypeStruct((1, rows), F32),
        ),
        in_specs=[hbm] * 4 + [smem] * 3,
        out_specs=(vmem, vmem, vmem),
        scratch_shapes=[
            pltpu.VMEM((seq, width), BF),
            pltpu.VMEM((seq, features), BF),
            pltpu.VMEM((seq, features), BF),
            pltpu.VMEM((rows, features), BF),
            pltpu.VMEM((width, features), BF),
            pltpu.VMEM((rows,), BF),
            pltpu.VMEM((width, features), F32),
            pltpu.VMEM((width, features), BF),
            pltpu.VMEM((count, pair, features), BF),
            pltpu.VMEM((2, max(count - 1, 1), pair, half), BF),
            pltpu.VMEM((2, max(count - 1, 1), pair, half), BF),
            pltpu.VMEM((chunks, chunk_rows, features), F32),
            pltpu.VMEM((2, chunks, chunk_rows, features), wire),
            pltpu.VMEM((2, chunks, chunk_rows, features), wire),
            pltpu.VMEM((some, count, part, features), BF),
            pltpu.VMEM((some, count, part, features), BF),
            pltpu.VMEM((some, rounds, part, features), BF),
            pltpu.VMEM((some, rounds, part, features), BF),
            pltpu.VMEM((chunks // 2, chunk_rows, features), F32),
            pltpu.VMEM((chunks // 2, chunk_rows, features), F32),
            pltpu.VMEM((len(stages), 1, 128), F32),
            pltpu.VMEM((2, 1, 128), F32),
            pltpu.VMEM((slots, 1, 128), F32),
            pltpu.VMEM((seq, features), F32),
            pltpu.VMEM((seq, 1), F32),
            pltpu.VMEM((rows, 1), F32),
            pltpu.VMEM((rows, 128), F32),
            dma((4,)),
            dma((10,)),
            dma((2 * count,)),
            dma((count,)),
            dma((2,)),
            dma((max(count // 2, 1) * chunks,)),
            dma((4 * (chunks - early),)),
            dma((some,)),
            dma((some * rounds,)),
            dma((chunks // 2,)),
            dma((1 + len(stages),)),
            pltpu.SemaphoreType.REGULAR,
        ],
        compiler_params=pltpu.CompilerParams(
            collective_id=0, has_side_effects=True, vmem_limit_bytes=40 * 1024 * 1024
        ),
    )(
        *[
            pltpu.with_memory_space_constraint(x, pltpu.HBM)
            for x in (states, cotangent, kv_weight, norm_gain)
        ],
        prompt_len, response_len, reward_bucket,
    )
    key_values, grad_weight, grad_gain = pl.pallas_call(
        writer,
        out_shape=(
            jax.ShapeDtypeStruct(key_values.shape, BF),
            jax.ShapeDtypeStruct(grad_weight.shape, F32),
            jax.ShapeDtypeStruct(grad_gain.shape, F32),
        ),
        in_specs=[vmem] * 3,
        out_specs=(hbm,) * 3,
        scratch_shapes=[dma((3,))],
    )(*[
        pltpu.with_memory_space_constraint(x, pltpu.VMEM)
        for x in (key_values, grad_weight, grad_gain)
    ])
    return key_values, grad_weight, grad_gain.reshape(rows)


def solution(mesh):
    placed = (
        P(("replica", "fsdp"), None, None),
        P(("replica", "fsdp"), None, None),
        P("fsdp", None),
        P("fsdp"),
        P(("replica", "fsdp")),
        P(("replica", "fsdp")),
        P(("replica", "fsdp")),
    )
    return jax.shard_map(
        functools.partial(shards, mesh.shape["replica"], mesh.shape["fsdp"]),
        mesh=mesh,
        in_specs=placed,
        out_specs=(P(("replica", "fsdp"), None, None), P("fsdp", None), P("fsdp")),
        check_vma=False,
    )
```
